16 devices in a mesh: dp: 2 (over y, z), tp: 8 (over x, core).
Axes of the slice: x: 4, y: 2, z: 1, core: 2. Of those that a mesh axis runs over, the one named last changes fastest.
The devices are a block of a 4x4x8 slice.
Arguments:
- x_in: bfloat16 [4, 1024, 3840], P('dp', 'tp'), parts along dimension 0
- positions: int32 [4, 1024], P('dp'), parts along dimension 0
- w_q: bfloat16 [3840, 16, 256], P(None, 'tp')
- w_k: bfloat16 [3840, 8, 256], P(None, 'tp')
- w_v: bfloat16 [3840, 8, 256], P(None, 'tp')
- w_o: bfloat16 [16, 256, 3840], P('tp')
- w_gate: bfloat16 [3840, 15360], P(None, 'tp')
- w_up: bfloat16 [3840, 15360], P(None, 'tp')
- w_down: bfloat16 [15360, 3840], P('tp')
- gain_attn: float32 [3840], replicated
- gain_mlp: float32 [3840], replicated
- d_out: bfloat16 [4, 1024, 3840], P('dp', 'tp'), parts along dimension 0
Outputs:
- output 1: bfloat16 [4, 1024, 3840], P('dp', 'tp'), parts along dimension 0
- output 2: bfloat16 [4, 1024, 3840], P('dp', 'tp'), parts along dimension 0
- output 3: bfloat16 [7680, 16, 256], P('dp', 'tp'), parts along dimension 0
- output 4: bfloat16 [7680, 8, 256], P('dp', 'tp'), parts along dimension 0
- output 5: bfloat16 [7680, 8, 256], P('dp', 'tp'), parts along dimension 0
- output 6: bfloat16 [32, 256, 3840], P(('dp', 'tp')), parts along dimension 0
- output 7: bfloat16 [7680, 15360], P('dp', 'tp'), parts along dimension 0
- output 8: bfloat16 [7680, 15360], P('dp', 'tp'), parts along dimension 0
- output 9: bfloat16 [30720, 3840], P(('dp', 'tp')), parts along dimension 0
- output 10: float32 [7680], P('dp'), parts along dimension 0
- output 11: float32 [7680], P('dp'), parts along dimension 0
There are 2 independent parts. The reference program is written for one: setup_inputs(seed, part) draws one part's arguments, and reference() takes and returns one part's arrays. A program takes and returns all parts, laid end to end along the dimension named above; an argument that names none is the same for every part.
All inputs are finite; a program needn't handle non-finite values.
Results may differ from the reference program's by a relative error of at most 0.02.
Values are sent between devices in bfloat16 or wider.
A program may use at most 768 MiB of HBM per device.

```python
import jax
import jax.numpy as jnp
from jax import lax

D = 3840
HEADS = 16
KV_HEADS = 8
HEAD = 256
FF = 15360
BATCH = 2
SEQ = 1024

EPS = 1e-6
ROPE_THETA = 10000.0


def setup_inputs(seed: int = 0, part: int = 0) -> dict:
    base_key = jax.random.key(seed)
    shared = jax.random.split(base_key, 9)
    own = jax.random.split(jax.random.fold_in(base_key, part), 4)
    x_in = jax.random.normal(own[0], (BATCH, SEQ, D), jnp.float32).astype(jnp.bfloat16)
    start_pos = jax.random.randint(own[1], (BATCH, 1), 0, 1024)
    steps = jax.random.randint(own[2], (BATCH, SEQ), 1, 5)
    positions = (start_pos + jnp.cumsum(steps, axis=1) - steps[:, :1]).astype(jnp.int32)
    d_out = jax.random.normal(own[3], (BATCH, SEQ, D), jnp.float32).astype(jnp.bfloat16)

    def weight(key_w, shape, fan_in):
        return (jax.random.normal(key_w, shape, jnp.float32) * fan_in ** -0.5).astype(jnp.bfloat16)

    return {
        "x_in": x_in,
        "positions": positions,
        "w_q": weight(shared[0], (D, HEADS, HEAD), D),
        "w_k": weight(shared[1], (D, KV_HEADS, HEAD), D),
        "w_v": weight(shared[2], (D, KV_HEADS, HEAD), D),
        "w_o": weight(shared[3], (HEADS, HEAD, D), HEADS * HEAD),
        "w_gate": weight(shared[4], (D, FF), D),
        "w_up": weight(shared[5], (D, FF), D),
        "w_down": weight(shared[6], (FF, D), FF),
        "gain_attn": 0.5 * jax.random.normal(shared[7], (D,), jnp.float32),
        "gain_mlp": 0.5 * jax.random.normal(shared[8], (D,), jnp.float32),
        "d_out": d_out,
    }


def rms_norm(vals, gain):
    vals_f32 = vals.astype(jnp.float32)
    inv_rms = lax.rsqrt(jnp.mean(vals_f32 * vals_f32, axis=-1, keepdims=True) + EPS)
    return (vals_f32 * inv_rms * (1.0 + gain)).astype(jnp.bfloat16)


def rope_tables(positions):
    half_dim = HEAD // 2
    inv_freq = ROPE_THETA ** (-2.0 * jnp.arange(half_dim, dtype=jnp.float32) / HEAD)
    angles = positions.astype(jnp.float32)[:, :, None] * inv_freq
    return jnp.cos(angles)[:, :, None, :], jnp.sin(angles)[:, :, None, :]


def apply_rope(heads_in, cos_t, sin_t):
    half_dim = heads_in.shape[-1] // 2
    vals_f32 = heads_in.astype(jnp.float32)
    first_half = vals_f32[..., :half_dim]
    second_half = vals_f32[..., half_dim:]
    return jnp.concatenate([first_half * cos_t - second_half * sin_t, second_half * cos_t + first_half * sin_t], axis=-1)


def attend_row(row_in):
    q_row, k_row, v_row = row_in
    seq_len = q_row.shape[0]
    groups = HEADS // KV_HEADS
    q_grp = q_row.astype(jnp.float32).reshape(seq_len, KV_HEADS, groups, HEAD)
    scores = jnp.einsum("qkgh,skh->kgqs", q_grp, k_row.astype(jnp.float32))
    causal = jnp.arange(seq_len)[:, None] >= jnp.arange(seq_len)[None, :]
    scores = jnp.where(causal, scores, -1e30)
    attn_probs = jax.nn.softmax(scores, axis=-1).astype(jnp.bfloat16)
    attn_rows = jnp.einsum("kgqs,skh->qkgh", attn_probs.astype(jnp.float32), v_row.astype(jnp.float32))
    return attn_rows.astype(jnp.bfloat16).reshape(seq_len, HEADS, HEAD)


def layer_forward(x_in, positions, w_q, w_k, w_v, w_o, w_gate, w_up, w_down, gain_attn, gain_mlp):
    cos_t, sin_t = rope_tables(positions)
    normed = rms_norm(x_in, gain_attn).astype(jnp.float32)
    q_raw = jnp.einsum("bsd,dnh->bsnh", normed, w_q).astype(jnp.bfloat16)
    k_raw = jnp.einsum("bsd,dnh->bsnh", normed, w_k).astype(jnp.bfloat16)
    v_raw = jnp.einsum("bsd,dnh->bsnh", normed, w_v).astype(jnp.bfloat16)
    q_rot = (apply_rope(q_raw, cos_t, sin_t) * HEAD ** -0.5).astype(jnp.bfloat16)
    k_rot = apply_rope(k_raw, cos_t, sin_t).astype(jnp.bfloat16)
    attn_out = lax.map(jax.checkpoint(attend_row), (q_rot, k_rot, v_raw))
    attn_proj = jnp.einsum("bsnh,nhd->bsd", attn_out.astype(jnp.float32), w_o).astype(jnp.bfloat16)
    hidden = (x_in.astype(jnp.float32) + attn_proj.astype(jnp.float32)).astype(jnp.bfloat16)
    mlp_in = rms_norm(hidden, gain_mlp).astype(jnp.float32)
    gate_pre = jnp.einsum("bsd,df->bsf", mlp_in, w_gate).astype(jnp.bfloat16)
    up_pre = jnp.einsum("bsd,df->bsf", mlp_in, w_up).astype(jnp.bfloat16)
    act_out = (jax.nn.gelu(gate_pre.astype(jnp.float32), approximate=True) * up_pre.astype(jnp.float32)).astype(jnp.bfloat16)
    down_out = jnp.einsum("bsf,fd->bsd", act_out.astype(jnp.float32), w_down).astype(jnp.bfloat16)
    return (hidden.astype(jnp.float32) + down_out.astype(jnp.float32)).astype(jnp.bfloat16)


def reference(x_in, positions, w_q, w_k, w_v, w_o, w_gate, w_up, w_down, gain_attn, gain_mlp, d_out):
    def forward(x_val, wq_f, wk_f, wv_f, wo_f, wg_f, wu_f, wd_f, gain_one, gain_two):
        return layer_forward(x_val, positions, wq_f, wk_f, wv_f, wo_f, wg_f, wu_f, wd_f, gain_one, gain_two)

    weights_f32 = [weight_mat.astype(jnp.float32) for weight_mat in (w_q, w_k, w_v, w_o, w_gate, w_up, w_down)]
    y_out, pullback = jax.vjp(forward, x_in, *weights_f32, gain_attn, gain_mlp)
    grads = pullback(d_out)
    return (
        y_out,
        grads[0],
        grads[1].astype(jnp.bfloat16),
        grads[2].astype(jnp.bfloat16),
        grads[3].astype(jnp.bfloat16),
        grads[4].astype(jnp.bfloat16),
        grads[5].astype(jnp.bfloat16),
        grads[6].astype(jnp.bfloat16),
        grads[7].astype(jnp.bfloat16),
        grads[8],
        grads[9],
    )
```

```python
import functools

import jax
import jax.numpy as jnp
from jax import lax
from jax.experimental import pallas as pl
from jax.experimental.pallas import tpu as pltpu
from jax.sharding import PartitionSpec as P

EPS = 1e-6
ROPE_THETA = 10000.0
BF = jnp.bfloat16
F32 = jnp.float32
GELU_C = 0.7978845608028654
GELU_A = 0.044715
VMEM_LIMIT = 60 * 1024 * 1024

NN = (((1,), (0,)), ((), ()))
NT = (((1,), (1,)), ((), ()))
TN = (((0,), (0,)), ((), ()))


def rms_norm(vals, gain):
    vals_f32 = vals.astype(F32)
    inv_rms = lax.rsqrt(jnp.mean(vals_f32 * vals_f32, axis=-1, keepdims=True) + EPS)
    return (vals_f32 * inv_rms * (1.0 + gain)).astype(BF)


def rope_tables(positions, head_dim):
    half_dim = head_dim // 2
    inv_freq = ROPE_THETA ** (-2.0 * jnp.arange(half_dim, dtype=F32) / head_dim)
    angles = positions.astype(F32)[:, :, None] * inv_freq
    return jnp.cos(angles), jnp.sin(angles)


def dot(lhs, rhs, dims):
    return lax.dot_general(lhs, rhs, dims, preferred_element_type=F32)


def after(value, *deps):
    return lax.optimization_barrier((value,) + deps)[0]


def join(parts, axis):
    return parts[0] if len(parts) == 1 else jnp.concatenate(parts, axis=axis)


def call(body, grid, in_specs, out_specs, out_shape, flops, nbytes, name, scratch=()):
    return pl.pallas_call(
        body,
        grid=grid,
        in_specs=in_specs,
        out_specs=out_specs,
        out_shape=out_shape,
        scratch_shapes=scratch,
        compiler_params=pltpu.CompilerParams(vmem_limit_bytes=VMEM_LIMIT),
        cost_estimate=pl.CostEstimate(flops=int(flops), bytes_accessed=int(nbytes), transcendentals=0),
        name=name,
    )


def whole(arr):
    zeros = (0,) * arr.ndim
    return pl.BlockSpec(arr.shape, lambda *_: zeros, pipeline_mode=pl.Buffered(1))


def rows_times_weights(acts, weights, kind, tile, name, m_tile=256):
    n_rows = acts[0].shape[0]
    nt = kind == "nt"
    n_cols = weights[0].shape[0 if nt else 1]
    depth = sum(a.shape[1] for a in acts)
    n_in = len(acts)
    grid = (pl.cdiv(n_cols, tile),)

    def body(*refs):
        a_refs, w_refs, out = refs[:n_in], refs[n_in:-1], refs[-1]
        rhs = join([w[...] for w in w_refs], 1 if nt else 0)
        for start in range(0, n_rows, m_tile):
            rows = pl.ds(start, m_tile)
            lhs = join([a[rows, :] for a in a_refs], 1)
            out[rows, :] = dot(lhs, rhs, NT if nt else NN).astype(BF)

    if nt:
        w_specs = [pl.BlockSpec((tile, w.shape[1]), lambda i: (i, 0)) for w in weights]
    else:
        w_specs = [pl.BlockSpec((w.shape[0], tile), lambda i: (0, i)) for w in weights]
    return call(
        body, grid, [whole(a) for a in acts] + w_specs,
        pl.BlockSpec((n_rows, tile), lambda i: (0, i)),
        jax.ShapeDtypeStruct((n_rows, n_cols), BF),
        2 * n_rows * depth * n_cols, 2 * (n_rows * depth + depth * n_cols + n_rows * n_cols), name,
    )(*acts, *weights)


def qkv_proj(acts, w_q, w_k, w_v):
    n_rows, depth = acts.shape
    m_tile = 256
    widths = (w_q.shape[1], w_k.shape[1], w_v.shape[1])

    def body(a_ref, wq, wk, wv, q, k, v):
        lhs = a_ref[...]
        q[...] = dot(lhs, wq[...], NN).astype(BF)
        kv = dot(lhs, jnp.concatenate([wk[...], wv[...]], axis=1), NN).astype(BF)
        k[...] = kv[:, : widths[1]]
        v[...] = kv[:, widths[1]:]

    return call(
        body, (n_rows // m_tile,),
        [pl.BlockSpec((m_tile, depth), lambda i: (i, 0)), whole(w_q), whole(w_k), whole(w_v)],
        [pl.BlockSpec((m_tile, w), lambda i: (i, 0)) for w in widths],
        [jax.ShapeDtypeStruct((n_rows, w), BF) for w in widths],
        2 * n_rows * depth * sum(widths), 2 * (n_rows * depth + depth * sum(widths) + n_rows * sum(widths)), "qkv",
    )(acts, w_q, w_k, w_v)


def rotate(vals, cos_t, sin_t):
    half = cos_t.shape[1]
    first, second = vals[:, :half].astype(F32), vals[:, half:].astype(F32)
    return jnp.concatenate([first * cos_t - second * sin_t, second * cos_t + first * sin_t], axis=1)


def unrotate(vals, cos_t, sin_t):
    half = cos_t.shape[1]
    first, second = vals[:, :half], vals[:, half:]
    return jnp.concatenate([first * cos_t + second * sin_t, second * cos_t - first * sin_t], axis=1)


def causal_probs(q_rows, k_rot, start, tile, n_rep):
    end = start + tile
    scores = dot(q_rows, k_rot[:end], NT)
    row = lax.broadcasted_iota(jnp.int32, (n_rep * tile, end), 0)
    col = lax.broadcasted_iota(jnp.int32, (n_rep * tile, end), 1)
    scores = jnp.where(lax.rem(row, tile) + start >= col, scores, -1e30)
    probs = jnp.exp(scores - jnp.max(scores, axis=1, keepdims=True))
    return probs / jnp.sum(probs, axis=1, keepdims=True)


def attention_fwd(q_raw, k_raw, v_raw, cos_t, sin_t, scale):
    n_rows, head = k_raw.shape
    n_rep = q_raw.shape[1] // head
    tile = 256

    def body(q, k, v, cos_ref, sin_ref, out, q_rot, k_rot):
        k_rot[...] = rotate(k[...], cos_ref[...], sin_ref[...]).astype(BF)
        for h in range(n_rep):
            cols = pl.ds(h * head, head)
            q_rot[:, cols] = (rotate(q[:, cols], cos_ref[...], sin_ref[...]) * scale).astype(BF)
        for start in range(0, n_rows, tile):
            rows = pl.ds(start, tile)
            q_rows = join([q_rot[rows, pl.ds(h * head, head)] for h in range(n_rep)], 0)
            probs = causal_probs(q_rows, k_rot, start, tile, n_rep).astype(BF)
            mixed = dot(probs, v[: start + tile], NN).astype(BF)
            for h in range(n_rep):
                out[rows, pl.ds(h * head, head)] = mixed[h * tile:(h + 1) * tile]

    ins = (q_raw, k_raw, v_raw, cos_t, sin_t)
    outs = [jax.ShapeDtypeStruct(a.shape, BF) for a in (q_raw, q_raw, k_raw)]
    return call(
        body, (1,), [whole(a) for a in ins], [whole(a) for a in outs], outs,
        4e9, 8e6, "attn_fwd",
    )(*ins)


def attention_bwd(q_rot, k_rot, v_raw, d_out, cos_t, sin_t, scale):
    n_rows, head = k_rot.shape
    n_rep = q_rot.shape[1] // head
    tile = 256

    def body(q, k, v, d_o, cos_ref, sin_ref, d_q, d_k, d_v, dk_acc, dv_acc):
        for start in reversed(range(0, n_rows, tile)):
            end = start + tile
            rows = pl.ds(start, tile)
            q_rows = join([q[rows, pl.ds(h * head, head)] for h in range(n_rep)], 0)
            do_rows = join([d_o[rows, pl.ds(h * head, head)] for h in range(n_rep)], 0)
            probs = causal_probs(q_rows, k, start, tile, n_rep)
            d_probs = dot(do_rows, v[:end], NT)
            d_scores = (probs * (d_probs - jnp.sum(d_probs * probs, axis=1, keepdims=True))).astype(BF)
            dv_part = dot(probs.astype(BF), do_rows, TN)
            dk_part = dot(d_scores, q_rows, TN)
            if end == n_rows:
                dv_acc[...] = dv_part
                dk_acc[...] = dk_part
            else:
                dv_acc[:end] += dv_part
                dk_acc[:end] += dk_part
            dq_rows = dot(d_scores, k[:end], NN).astype(BF).astype(F32) * scale
            for h in range(n_rep):
                part = dq_rows[h * tile:(h + 1) * tile]
                d_q[rows, pl.ds(h * head, head)] = unrotate(part, cos_ref[rows, :], sin_ref[rows, :]).astype(BF)
        d_v[...] = dv_acc[...].astype(BF)
        d_k[...] = unrotate(dk_acc[...].astype(BF).astype(F32), cos_ref[...], sin_ref[...]).astype(BF)

    ins = (q_rot, k_rot, v_raw, d_out, cos_t, sin_t)
    outs = [jax.ShapeDtypeStruct(a.shape, BF) for a in (q_rot, k_rot, v_raw)]
    return call(
        body, (1,), [whole(a) for a in ins], [whole(a) for a in outs], outs,
        8e9, 8e6, "attn_bwd", [pltpu.VMEM((n_rows, head), F32)] * 2,
    )(*ins)


def gated_mlp(acts, w_gate, w_up, d_act):
    n_rows, depth = acts.shape
    width = w_gate.shape[1]
    tile, m_tile = 384, 256

    def body(a_ref, wg, wu, dz_ref, z_ref, dg_ref, du_ref):
        rhs = jnp.concatenate([wg[...], wu[...]], axis=1)
        for start in range(0, n_rows, m_tile):
            rows = pl.ds(start, m_tile)
            both = dot(a_ref[rows, :], rhs, NN)
            gate = both[:, :tile].astype(BF).astype(F32)
            up = both[:, tile:].astype(BF).astype(F32)
            d_z = dz_ref[rows, :].astype(F32)
            square = gate * gate
            tanh = jnp.tanh(gate * (GELU_C + (GELU_C * GELU_A) * square))
            half = 0.5 + 0.5 * tanh
            act = gate * half
            slope = half + (0.5 * gate) * (1.0 - tanh * tanh) * (GELU_C + (3.0 * GELU_C * GELU_A) * square)
            z_ref[rows, :] = (act * up).astype(BF)
            du_ref[rows, :] = (d_z * act).astype(BF)
            dg_ref[rows, :] = (d_z * up * slope).astype(BF)

    w_spec = pl.BlockSpec((depth, tile), lambda i: (0, i))
    o_spec = pl.BlockSpec((n_rows, tile), lambda i: (0, i))
    return call(
        body, (width // tile,), [whole(acts), w_spec, w_spec, o_spec], [o_spec] * 3,
        [jax.ShapeDtypeStruct((n_rows, width), BF)] * 3,
        4 * n_rows * depth * width, 2 * (n_rows * depth + 2 * depth * width + 4 * n_rows * width), "gated_mlp",
    )(acts, w_gate, w_up, d_act)


def weight_grad(lhs, rhs_groups, out_widths, tile, name, stream):
    n_seq, n_tok = len(lhs), lhs[0].shape[0]
    n_out = lhs[0].shape[1]
    rhs = [r for group in rhs_groups for r in group]
    n_groups = len(rhs_groups)

    def body(*refs):
        l_refs, r_refs, o_refs = refs[:n_seq], refs[n_seq:n_seq + n_seq * n_groups], refs[n_seq + n_seq * n_groups:]
        left = join([l[...] for l in l_refs], 0)
        right = join([join([r_refs[g * n_seq + s][...] for s in range(n_seq)], 0) for g in range(n_groups)], 1)
        acc = dot(left, right, TN)
        at = 0
        for o in o_refs:
            o[...] = acc[:, at:at + o.shape[1]].astype(BF)
            at += o.shape[1]

    if stream == "rows":
        grid = (n_out // tile,)
        l_specs = [pl.BlockSpec((n_tok, tile), lambda i: (0, i)) for _ in lhs]
        r_specs = [whole(r) for r in rhs]
        o_specs = [pl.BlockSpec((tile, w), lambda i: (i, 0)) for w in out_widths]
    else:
        grid = (out_widths[0] // tile,)
        l_specs = [whole(l) for l in lhs]
        r_specs = [pl.BlockSpec((n_tok, tile), lambda i: (0, i)) for _ in rhs]
        o_specs = [pl.BlockSpec((n_out, tile), lambda i: (0, i)) for _ in out_widths]
    total = sum(out_widths)
    return call(
        body, grid, l_specs + r_specs, o_specs,
        [jax.ShapeDtypeStruct((n_out, w), BF) for w in out_widths],
        2 * n_seq * n_tok * n_out * total, 2 * (n_seq * n_tok * (n_out + total) + n_out * total), name,
    )(*lhs, *rhs)


def tp_sum(part, n_tp):
    def body(x_ref, out_ref, slots, send_sem, recv_sem):
        me = lax.axis_index("tp")
        barrier = pltpu.get_barrier_semaphore()
        for step in range(1, n_tp):
            pl.semaphore_signal(barrier, inc=1, device_id={"tp": lax.rem(me + step, n_tp)},
                                device_id_type=pl.DeviceIdType.MESH)
        pl.semaphore_wait(barrier, n_tp - 1)
        copies = []
        for step in range(1, n_tp):
            copies.append(pltpu.make_async_remote_copy(
                src_ref=x_ref, dst_ref=slots.at[me], send_sem=send_sem.at[step], recv_sem=recv_sem.at[step],
                device_id={"tp": lax.rem(me + step, n_tp)}, device_id_type=pl.DeviceIdType.MESH))
            copies[-1].start()
        slots[me] = x_ref[...]
        for copy in copies:
            copy.wait()
        total = slots[0]
        for step in range(1, n_tp):
            total = total + slots[step]
        out_ref[...] = total

    return pl.pallas_call(
        body,
        out_shape=jax.ShapeDtypeStruct(part.shape, F32),
        in_specs=[pl.BlockSpec(memory_space=pltpu.VMEM)],
        out_specs=pl.BlockSpec(memory_space=pltpu.VMEM),
        scratch_shapes=[pltpu.VMEM((n_tp,) + part.shape, F32), pltpu.SemaphoreType.DMA((n_tp,)),
                        pltpu.SemaphoreType.DMA((n_tp,))],
        compiler_params=pltpu.CompilerParams(collective_id=0, has_side_effects=True),
        cost_estimate=pl.CostEstimate(flops=5_000_000_000, bytes_accessed=1_000_000, transcendentals=0),
        name="tp_sum",
    )(part)


def solution(mesh):
    n_tp = mesh.shape["tp"]
    act_spec = P("dp", "tp", None)
    head_spec = P(None, "tp", None)
    in_specs = (act_spec, P("dp", None), head_spec, head_spec, head_spec, P("tp", None, None),
                P(None, "tp"), P(None, "tp"), P("tp", None), P(None), P(None), act_spec)
    out_specs = (act_spec, act_spec, P("dp", "tp", None), P("dp", "tp", None), P("dp", "tp", None),
                 P(("dp", "tp"), None, None), P("dp", "tp"), P("dp", "tp"), P(("dp", "tp"), None), P("dp"), P("dp"))

    def gather(part):
        return lax.all_gather(part, "tp", axis=0, tiled=True)

    def scatter(part):
        return lax.psum_scatter(part, "tp", scatter_dimension=0, tiled=True)

    def local_step(x_in, positions, w_q, w_k, w_v, w_o, w_gate, w_up, w_down, gain_attn, gain_mlp, d_out):
        n_seq = x_in.shape[0]
        seqs = range(n_seq)
        depth, n_q, head = w_q.shape
        scale = head ** -0.5
        wq2, wk2, wv2 = (w.reshape(depth, -1) for w in (w_q, w_k, w_v))
        wo2 = w_o.reshape(-1, depth)
        cos_t, sin_t = rope_tables(positions, head)

        x = [x_in[s] for s in seqs]
        d_y = [d_out[s] for s in seqs]
        latest = []

        def run(fn, first, *rest):
            out = fn(after(first, *latest), *rest)
            latest[:] = jax.tree.leaves(out)[:1]
            return out

        def norm(vals, gain):
            return jax.vjp(rms_norm, vals, gain)

        def mid_norm(proj, vals):
            total = (vals.astype(F32) + proj.astype(F32)).astype(BF)
            return norm(total, gain_mlp) + (total,)

        def project(acts):
            return qkv_proj(acts, wq2, wk2, wv2)

        def attend(q_raw, k_raw, v_raw, s):
            return attention_fwd(q_raw, k_raw, v_raw, cos_t[s], sin_t[s], scale)

        def out_proj(acts):
            return rows_times_weights([acts], [wo2], "nn", 768, "o_proj")

        def act_grad(cot):
            return rows_times_weights([cot], [w_down], "nt", 1024, "d_act")

        def mlp_grad(d_g, d_u):
            return rows_times_weights([d_g, d_u], [w_gate, w_up], "nt", 768, "d_mlp")

        def down_proj(acts):
            return rows_times_weights([acts], [w_down], "nn", 768, "down")

        def norm_back(cot, pull, skip):
            d_vals, d_gain = pull(cot)
            return skip + d_vals, d_gain

        def attn_grads(cot, s):
            d_o = rows_times_weights([cot], [wo2], "nt", 256, "d_attn")
            grads = attention_bwd(attn[s][1], attn[s][2], qkv[s][2], d_o, cos_t[s], sin_t[s], scale)
            part = rows_times_weights(list(grads), [wq2, wk2, wv2], "nt", 768, "d_normed")
            return part, grads

        def add_out(part, vals):
            return (vals.astype(F32) + part.astype(F32)).astype(BF)

        none = [None] * n_seq
        normed_all, dout_all, qkv, attn, attn_proj, mlp_all = (list(none) for _ in range(6))
        norm_attn_pull, norm_mlp_pull, hidden, d_act, gated, d_mlp_in = (list(none) for _ in range(6))
        down_out, d_hidden, gain_mlp_part, d_hidden_all, d_qkv, d_normed = (list(none) for _ in range(6))
        grad_x, gain_attn_part, y_out = (list(none) for _ in range(3))

        for s in seqs:
            out, norm_attn_pull[s] = run(norm, x[s], gain_attn)
            normed_all[s] = gather(out)
        for s in seqs:
            qkv[s] = run(project, normed_all[s])
            attn[s] = run(attend, *qkv[s], s)
            attn_proj[s] = scatter(run(out_proj, attn[s][0]))
        dout_all[0] = gather(after(d_y[0], *latest))
        for s in seqs:
            out, norm_mlp_pull[s], hidden[s] = run(mid_norm, attn_proj[s], x[s])
            mlp_all[s] = gather(out)
        for s in seqs[1:]:
            dout_all[s] = gather(after(d_y[s], *latest))

        def mlp_half(s):
            d_act[s] = run(act_grad, dout_all[s])
            gated[s] = run(gated_mlp, mlp_all[s], w_gate, w_up, d_act[s])

        def mlp_rest(s):
            d_mlp_in[s] = scatter(run(mlp_grad, gated[s][1], gated[s][2]))
            down_out[s] = scatter(run(down_proj, gated[s][0]))

        def mid_back(s):
            d_hidden[s], gain_mlp_part[s] = run(norm_back, d_mlp_in[s], norm_mlp_pull[s], d_y[s])
            d_hidden_all[s] = gather(d_hidden[s])

        def attn_back(s):
            part, d_qkv[s] = run(attn_grads, d_hidden_all[s], s)
            d_normed[s] = scatter(part)

        def last_back(s):
            grad_x[s], gain_attn_part[s] = run(norm_back, d_normed[s], norm_attn_pull[s], d_hidden[s])

        mlp_half(0)
        mlp_rest(0)
        mlp_half(1)
        mid_back(0)
        mlp_rest(1)
        y_out[0] = run(add_out, down_out[0], hidden[0])
        act_out, d_gate, d_up = zip(*gated)
        (grad_wdown,) = run(lambda first: weight_grad([first, act_out[1]], [dout_all], (depth,), 768, "g_down", "cols"),
                            act_out[0])
        attn_back(0)
        mid_back(1)
        grad_wgate, grad_wup = run(lambda first: weight_grad(
            [first, mlp_all[1]], [d_gate, d_up], (w_gate.shape[1],) * 2, 384, "g_gate_up", "rows"), mlp_all[0])
        attn_back(1)
        (grad_wo,) = run(lambda first: weight_grad([first, attn[1][0]], [d_hidden_all], (depth,), 768, "g_o", "cols"),
                         attn[0][0])
        d_q, d_k, d_v = zip(*d_qkv)
        grad_wq, grad_wk, grad_wv = run(lambda first: weight_grad(
            [first, normed_all[1]], [d_q, d_k, d_v], tuple(w.shape[1] for w in (wq2, wk2, wv2)), 384, "g_qkv", "rows"),
            normed_all[0])
        last_back(0)
        y_out[1] = run(add_out, down_out[1], hidden[1])
        last_back(1)
        back_attn, back_mlp = gain_attn_part, gain_mlp_part
        gain_parts = jnp.stack([functools.reduce(jnp.add, back) for back in (back_attn, back_mlp)])
        gains = tp_sum(gain_parts, n_tp)
        return (jnp.stack(y_out), jnp.stack(grad_x), grad_wq.reshape(w_q.shape), grad_wk.reshape(w_k.shape),
                grad_wv.reshape(w_v.shape), grad_wo.reshape(w_o.shape), grad_wgate, grad_wup, grad_wdown,
                gains[0], gains[1])

    return jax.shard_map(local_step, mesh=mesh, in_specs=in_specs, out_specs=out_specs, check_vma=False)
```

```python
import functools

import jax
import jax.numpy as jnp
from jax import lax
from jax.experimental import pallas as pl
from jax.experimental.pallas import tpu as pltpu
from jax.sharding import PartitionSpec as P


EPS = 1e-6
ROPE_THETA = 10000.0
BF = jnp.bfloat16
F32 = jnp.float32
GELU_C = 0.7978845608028654
GELU_A = 0.044715
VMEM_LIMIT = 60 * 1024 * 1024

NN = (((1,), (0,)), ((), ()))
NT = (((1,), (1,)), ((), ()))
TN = (((0,), (0,)), ((), ()))


def rms_norm(vals, gain):
    vals_f32 = vals.astype(F32)
    inv_rms = lax.rsqrt(jnp.mean(vals_f32 * vals_f32, axis=-1, keepdims=True) + EPS)
    return (vals_f32 * inv_rms * (1.0 + gain)).astype(BF)


def rope_tables(positions, head_dim):
    half_dim = head_dim // 2
    inv_freq = ROPE_THETA ** (-2.0 * jnp.arange(half_dim, dtype=F32) / head_dim)
    angles = positions.astype(F32)[:, :, None] * inv_freq
    return jnp.cos(angles), jnp.sin(angles)


def dot(lhs, rhs, dims):
    return lax.dot_general(lhs, rhs, dims, preferred_element_type=F32)


def after(value, *deps):
    return lax.optimization_barrier((value,) + deps)[0]


def join(parts, axis):
    return parts[0] if len(parts) == 1 else jnp.concatenate(parts, axis=axis)


def call(body, grid, in_specs, out_specs, out_shape, flops, nbytes, scratch=()):
    return pl.pallas_call(
        body,
        grid=grid,
        in_specs=in_specs,
        out_specs=out_specs,
        out_shape=out_shape,
        scratch_shapes=scratch,
        compiler_params=pltpu.CompilerParams(vmem_limit_bytes=VMEM_LIMIT),
        cost_estimate=pl.CostEstimate(flops=int(flops), bytes_accessed=int(nbytes), transcendentals=0),
    )


def whole(arr):
    zeros = (0,) * arr.ndim
    return pl.BlockSpec(arr.shape, lambda *_: zeros, pipeline_mode=pl.Buffered(1))


def rows_times_weights(acts, weights, kind, tile, m_tile=256):
    n_rows = acts[0].shape[0]
    nt = kind == "nt"
    n_cols = weights[0].shape[0 if nt else 1]
    depth = sum(a.shape[1] for a in acts)
    n_in = len(acts)
    grid = (pl.cdiv(n_cols, tile),)

    def body(*refs):
        a_refs, w_refs, out = refs[:n_in], refs[n_in:-1], refs[-1]
        rhs = join([w[...] for w in w_refs], 1 if nt else 0)
        for start in range(0, n_rows, m_tile):
            rows = pl.ds(start, m_tile)
            lhs = join([a[rows, :] for a in a_refs], 1)
            out[rows, :] = dot(lhs, rhs, NT if nt else NN).astype(BF)

    if nt:
        w_specs = [pl.BlockSpec((tile, w.shape[1]), lambda i: (i, 0)) for w in weights]
    else:
        w_specs = [pl.BlockSpec((w.shape[0], tile), lambda i: (0, i)) for w in weights]
    return call(
        body, grid, [whole(a) for a in acts] + w_specs,
        pl.BlockSpec((n_rows, tile), lambda i: (0, i)),
        jax.ShapeDtypeStruct((n_rows, n_cols), BF),
        2 * n_rows * depth * n_cols, 2 * (n_rows * depth + depth * n_cols + n_rows * n_cols),
    )(*acts, *weights)


def rotate(vals, cos_t, sin_t):
    half = cos_t.shape[1]
    first, second = vals[:, :half].astype(F32), vals[:, half:].astype(F32)
    return jnp.concatenate([first * cos_t - second * sin_t, second * cos_t + first * sin_t], axis=1)


def unrotate(vals, cos_t, sin_t):
    half = cos_t.shape[1]
    first, second = vals[:, :half], vals[:, half:]
    return jnp.concatenate([first * cos_t + second * sin_t, second * cos_t - first * sin_t], axis=1)


def causal_probs(q_rows, k_rot, start, tile, n_rep):
    end = start + tile
    scores = dot(q_rows, k_rot[:end], NT)
    row = lax.broadcasted_iota(jnp.int32, (n_rep * tile, end), 0)
    col = lax.broadcasted_iota(jnp.int32, (n_rep * tile, end), 1)
    scores = jnp.where(lax.rem(row, tile) + start >= col, scores, -1e30)
    probs = jnp.exp(scores - jnp.max(scores, axis=1, keepdims=True))
    return probs / jnp.sum(probs, axis=1, keepdims=True)


def attention_fwd(acts, w_qkv, w_o, cos_t, sin_t, n_rep, head, scale):
    n_rows, depth = acts.shape
    n_q, width = n_rep * head, w_qkv.shape[1]
    tile = 256
    n_tiles, n_cols = n_rows // tile, width // tile

    def body(acts_hbm, w_hbm, wo_hbm, cos_ref, sin_ref, q_rot, k_rot, v, out, part_hbm,
             acts_v, w_v, wo_v, qkv, part_v, a_sem, w_sem, wo_sem, o_sem):
        a_copy = [pltpu.make_async_copy(acts_hbm.at[pl.ds(i * tile, tile)], acts_v.at[pl.ds(i * tile, tile)],
                                        a_sem.at[i]) for i in range(n_tiles)]
        w_copy = [pltpu.make_async_copy(w_hbm.at[:, pl.ds(i * tile, tile)], w_v.at[:, pl.ds(i * tile, tile)],
                                        w_sem.at[i]) for i in range(n_cols)]
        wo_copy = pltpu.make_async_copy(wo_hbm, wo_v, wo_sem)
        o_copy = [pltpu.make_async_copy(part_v.at[i % 2], part_hbm.at[pl.ds(i * tile, tile)], o_sem.at[i % 2])
                  for i in range(n_tiles)]
        for copy in a_copy[:1] + w_copy + [wo_copy] + a_copy[1:]:
            copy.start()
        for i in range(n_tiles):
            rows = pl.ds(i * tile, tile)
            a_copy[i].wait()
            if i == 0:
                for j in range(n_cols):
                    w_copy[j].wait()
                    cols = pl.ds(j * tile, tile)
                    qkv[:, cols] = dot(acts_v[rows, :], w_v[:, cols], NN).astype(BF)
                wo_copy.wait()
            else:
                qkv[...] = dot(acts_v[rows, :], w_v[...], NN).astype(BF)
            cos, sin = cos_ref[rows, :], sin_ref[rows, :]
            k_rot[rows, :] = rotate(qkv[:, n_q:n_q + head], cos, sin).astype(BF)
            v[rows, :] = qkv[:, n_q + head:]
            q_rows = join([(rotate(qkv[:, h * head:(h + 1) * head], cos, sin) * scale).astype(BF)
                           for h in range(n_rep)], 0)
            probs = causal_probs(q_rows, k_rot, i * tile, tile, n_rep).astype(BF)
            mixed = dot(probs, v[: (i + 1) * tile], NN).astype(BF)
            for h in range(n_rep):
                cols = pl.ds(h * head, head)
                q_rot[rows, cols] = q_rows[h * tile:(h + 1) * tile]
                out[rows, cols] = mixed[h * tile:(h + 1) * tile]
            if i >= 2:
                o_copy[i].wait()
            heads = join([mixed[h * tile:(h + 1) * tile] for h in range(n_rep)], 1)
            part_v[i % 2] = dot(heads, wo_v[...], NN).astype(BF)
            o_copy[i].start()
        for i in range(max(0, n_tiles - 2), n_tiles):
            o_copy[i].wait()

    any_spec = pl.BlockSpec(memory_space=pl.ANY)
    outs = [jax.ShapeDtypeStruct((n_rows, w), BF) for w in (n_q, head, head, n_q)]
    return call(
        body, (1,), [any_spec] * 3 + [whole(cos_t), whole(sin_t)], [whole(o) for o in outs] + [any_spec],
        outs + [jax.ShapeDtypeStruct((n_rows, depth), BF)],
        2 * n_rows * depth * (width + n_q) + 4e9, 2 * (2 * n_rows * depth + depth * (width + n_q)),
        [pltpu.VMEM((n_rows, depth), BF), pltpu.VMEM(w_qkv.shape, BF), pltpu.VMEM(w_o.shape, BF),
         pltpu.VMEM((tile, width), BF), pltpu.VMEM((2, tile, depth), BF),
         pltpu.SemaphoreType.DMA((n_tiles,)), pltpu.SemaphoreType.DMA((n_cols,)), pltpu.SemaphoreType.DMA,
         pltpu.SemaphoreType.DMA((2,))],
    )(acts, w_qkv, w_o, cos_t, sin_t)


def attention_bwd(cot, w_qkv, w_o, q_rot, k_rot, v_raw, cos_t, sin_t, scale):
    n_rows, depth = cot.shape
    head = k_rot.shape[1]
    n_q, width = q_rot.shape[1], w_qkv.shape[1]
    n_rep = n_q // head
    tile = 256
    n_tiles = n_rows // tile

    def body(cot_hbm, w_hbm, wo_hbm, q, k, v, cos_ref, sin_ref, d_qkv, part_hbm,
             cot_v, w_v, wo_v, part_v, dk_acc, dv_acc, c_sem, w_sem, wo_sem, o_sem):
        order = list(reversed(range(n_tiles)))
        c_copy = [pltpu.make_async_copy(cot_hbm.at[pl.ds(i * tile, tile)], cot_v.at[pl.ds(i * tile, tile)],
                                        c_sem.at[i]) for i in range(n_tiles)]
        w_copy = pltpu.make_async_copy(w_hbm, w_v, w_sem)
        wo_copy = pltpu.make_async_copy(wo_hbm, wo_v, wo_sem)
        o_copy = [pltpu.make_async_copy(part_v.at[i % 2], part_hbm.at[pl.ds(i * tile, tile)], o_sem.at[i % 2])
                  for i in range(n_tiles)]
        for copy in [wo_copy] + [c_copy[i] for i in order[:1]] + [w_copy] + [c_copy[i] for i in order[1:]]:
            copy.start()
        wo_copy.wait()
        for n, i in enumerate(order):
            rows, end = pl.ds(i * tile, tile), (i + 1) * tile
            c_copy[i].wait()
            d_o = dot(cot_v[rows, :], wo_v[...], NT).astype(BF)
            q_rows = join([q[rows, pl.ds(h * head, head)] for h in range(n_rep)], 0)
            do_rows = join([d_o[:, h * head:(h + 1) * head] for h in range(n_rep)], 0)
            probs = causal_probs(q_rows, k, i * tile, tile, n_rep)
            d_probs = dot(do_rows, v[:end], NT)
            d_scores = (probs * (d_probs - jnp.sum(d_probs * probs, axis=1, keepdims=True))).astype(BF)
            dv_part = dot(probs.astype(BF), do_rows, TN)
            dk_part = dot(d_scores, q_rows, TN)
            if n == 0:
                dv_acc[...] = dv_part
                dk_acc[...] = dk_part
            else:
                dv_acc[:end] += dv_part
                dk_acc[:end] += dk_part
            dq_rows = dot(d_scores, k[:end], NN).astype(BF).astype(F32) * scale
            cos, sin = cos_ref[rows, :], sin_ref[rows, :]
            parts = [unrotate(dq_rows[h * tile:(h + 1) * tile], cos, sin).astype(BF) for h in range(n_rep)]
            parts.append(unrotate(dk_acc[rows, :].astype(BF).astype(F32), cos, sin).astype(BF))
            parts.append(dv_acc[rows, :].astype(BF))
            tile_grad = join(parts, 1)
            d_qkv[rows, :] = tile_grad
            if n == 0:
                w_copy.wait()
            if n >= 2:
                o_copy[i].wait()
            part_v[i % 2] = dot(tile_grad, w_v[...], NT).astype(BF)
            o_copy[i].start()
        for i in order[-2:]:
            o_copy[i].wait()

    any_spec = pl.BlockSpec(memory_space=pl.ANY)
    rest = (q_rot, k_rot, v_raw, cos_t, sin_t)
    outs = [jax.ShapeDtypeStruct((n_rows, width), BF), jax.ShapeDtypeStruct((n_rows, depth), BF)]
    return call(
        body, (1,), [any_spec] * 3 + [whole(r) for r in rest], [whole(outs[0]), any_spec], outs,
        2 * n_rows * depth * (width + n_q) + 8e9, 2 * (2 * n_rows * depth + depth * (width + n_q)),
        [pltpu.VMEM((n_rows, depth), BF), pltpu.VMEM(w_qkv.shape, BF), pltpu.VMEM(w_o.shape, BF),
         pltpu.VMEM((2, tile, depth), BF), pltpu.VMEM((n_rows, head), F32), pltpu.VMEM((n_rows, head), F32),
         pltpu.SemaphoreType.DMA((n_tiles,)), pltpu.SemaphoreType.DMA, pltpu.SemaphoreType.DMA,
         pltpu.SemaphoreType.DMA((2,))],
    )(cot, w_qkv, w_o, *rest)


def aligned(offset):
    return pl.multiple_of(offset, 128)


def act_cotangent(pieces, offsets, seq, w_down, tile):
    width, depth = w_down.shape
    n_rows = sum(p.shape[1] for p in pieces)

    def body(off_ref, *refs):
        p_refs, w_ref, out = refs[:-2], refs[-2], refs[-1]
        rhs = w_ref[...]
        groups = [[0], [1], [2], [3, 4]]
        for group in groups:
            vals = dot(join([p_refs[g][...] for g in group], 0), rhs, NT).astype(BF)
            at = 0
            for g in group:
                size = p_refs[g].shape[0]
                out[pl.ds(aligned(off_ref[g]), size), :] = vals[at:at + size]
                at += size

    p_specs = [pl.BlockSpec((None,) + p.shape[1:], lambda i: (seq, 0, 0), pipeline_mode=pl.Buffered(1)) for p in pieces]
    return call(
        body, (pl.cdiv(width, tile),),
        [pl.BlockSpec(memory_space=pltpu.SMEM)] + p_specs + [pl.BlockSpec((tile, depth), lambda i: (i, 0))],
        pl.BlockSpec((n_rows, tile), lambda i: (0, i)), jax.ShapeDtypeStruct((n_rows, width), BF),
        2 * n_rows * depth * width, 2 * (n_rows * depth + depth * width + n_rows * width),
    )(offsets, *pieces, w_down)


def down_grad(acts, pieces, offsets, tile):
    n_seq = len(acts)
    n_tok, width = acts[0].shape
    depth = pieces[0].shape[2]

    def body(off_ref, *refs):
        z_refs, p_refs, out = refs[:n_seq], refs[n_seq:-1], refs[-1]
        left = join([z[pl.ds(aligned(off_ref[g]), p.shape[1]), :] for z in z_refs for g, p in enumerate(p_refs)], 0)
        right = join([p[s] for s in range(n_seq) for p in p_refs], 0)
        out[...] = dot(left, right, TN).astype(BF)

    p_specs = [pl.BlockSpec(p.shape[:2] + (tile,), lambda i: (0, 0, i)) for p in pieces]
    return call(
        body, (depth // tile,),
        [pl.BlockSpec(memory_space=pltpu.SMEM)] + [whole(z) for z in acts] + p_specs,
        pl.BlockSpec((width, tile), lambda i: (0, i)), jax.ShapeDtypeStruct((width, depth), BF),
        2 * n_seq * n_tok * width * depth, 2 * (n_seq * n_tok * (width + depth) + width * depth),
    )(offsets, *acts, *pieces)


def gated_mlp(acts, w_gate, w_up, d_act):
    n_rows, depth = acts.shape
    width = w_gate.shape[1]
    tile, m_tile = 384, 256

    def body(a_ref, wg, wu, dz_ref, z_ref, dg_ref, du_ref):
        rhs = jnp.concatenate([wg[...], wu[...]], axis=1)
        for start in range(0, n_rows, m_tile):
            rows = pl.ds(start, m_tile)
            both = dot(a_ref[rows, :], rhs, NN)
            gate = both[:, :tile].astype(BF).astype(F32)
            up = both[:, tile:].astype(BF).astype(F32)
            d_z = dz_ref[rows, :].astype(F32)
            square = gate * gate
            tanh = jnp.tanh(gate * (GELU_C + (GELU_C * GELU_A) * square))
            half = 0.5 + 0.5 * tanh
            act = gate * half
            slope = half + (0.5 * gate) * (1.0 - tanh * tanh) * (GELU_C + (3.0 * GELU_C * GELU_A) * square)
            z_ref[rows, :] = (act * up).astype(BF)
            du_ref[rows, :] = (d_z * act).astype(BF)
            dg_ref[rows, :] = (d_z * up * slope).astype(BF)

    w_spec = pl.BlockSpec((depth, tile), lambda i: (0, i))
    o_spec = pl.BlockSpec((n_rows, tile), lambda i: (0, i))
    return call(
        body, (width // tile,), [whole(acts), w_spec, w_spec, o_spec], [o_spec] * 3,
        [jax.ShapeDtypeStruct((n_rows, width), BF)] * 3,
        4 * n_rows * depth * width, 2 * (n_rows * depth + 2 * depth * width + 4 * n_rows * width),
    )(acts, w_gate, w_up, d_act)


def weight_grad(lhs, rhs_groups, out_widths, tile, stream):
    n_seq, n_tok = len(lhs), lhs[0].shape[0]
    n_out = lhs[0].shape[1]
    rhs = [r for group in rhs_groups for r in group]
    n_groups = len(rhs_groups)

    def body(*refs):
        l_refs, r_refs, o_refs = refs[:n_seq], refs[n_seq:n_seq + n_seq * n_groups], refs[n_seq + n_seq * n_groups:]
        left = join([l[...] for l in l_refs], 0)
        right = join([join([r_refs[g * n_seq + s][...] for s in range(n_seq)], 0) for g in range(n_groups)], 1)
        acc = dot(left, right, TN)
        at = 0
        for o in o_refs:
            o[...] = acc[:, at:at + o.shape[1]].astype(BF)
            at += o.shape[1]

    if stream == "rows":
        grid = (n_out // tile,)
        l_specs = [pl.BlockSpec((n_tok, tile), lambda i: (0, i)) for _ in lhs]
        r_specs = [whole(r) for r in rhs]
        o_specs = [pl.BlockSpec((tile, w), lambda i: (i, 0)) for w in out_widths]
    else:
        grid = (out_widths[0] // tile,)
        l_specs = [whole(l) for l in lhs]
        r_specs = [pl.BlockSpec((n_tok, tile), lambda i: (0, i)) for _ in rhs]
        o_specs = [pl.BlockSpec((n_out, tile), lambda i: (0, i)) for _ in out_widths]
    total = sum(out_widths)
    return call(
        body, grid, l_specs + r_specs, o_specs,
        [jax.ShapeDtypeStruct((n_out, w), BF) for w in out_widths],
        2 * n_seq * n_tok * n_out * total, 2 * (n_seq * n_tok * (n_out + total) + n_out * total),
    )(*lhs, *rhs)


def tp_sum(part, n_tp):
    def body(x_ref, out_ref, slots, send_sem, recv_sem):
        me = lax.axis_index("tp")
        barrier = pltpu.get_barrier_semaphore()
        for step in range(1, n_tp):
            pl.semaphore_signal(barrier, inc=1, device_id={"tp": lax.rem(me + step, n_tp)},
                                device_id_type=pl.DeviceIdType.MESH)
        pl.semaphore_wait(barrier, n_tp - 1)
        copies = []
        for step in range(1, n_tp):
            copies.append(pltpu.make_async_remote_copy(
                src_ref=x_ref, dst_ref=slots.at[me], send_sem=send_sem.at[step], recv_sem=recv_sem.at[step],
                device_id={"tp": lax.rem(me + step, n_tp)}, device_id_type=pl.DeviceIdType.MESH))
            copies[-1].start()
        slots[me] = x_ref[...]
        for copy in copies:
            copy.wait()
        total = slots[0]
        for step in range(1, n_tp):
            total = total + slots[step]
        out_ref[...] = total

    return pl.pallas_call(
        body,
        out_shape=jax.ShapeDtypeStruct(part.shape, F32),
        in_specs=[pl.BlockSpec(memory_space=pltpu.VMEM)],
        out_specs=pl.BlockSpec(memory_space=pltpu.VMEM),
        scratch_shapes=[pltpu.VMEM((n_tp,) + part.shape, F32), pltpu.SemaphoreType.DMA((n_tp,)),
                        pltpu.SemaphoreType.DMA((n_tp,))],
        compiler_params=pltpu.CompilerParams(collective_id=0, has_side_effects=True),
        cost_estimate=pl.CostEstimate(flops=5_000_000_000, bytes_accessed=1_000_000, transcendentals=0),
        name="tp_sum",
    )(part)


def solution(mesh):
    n_tp = mesh.shape["tp"]
    act_spec = P("dp", "tp", None)
    head_spec = P(None, "tp", None)
    in_specs = (act_spec, P("dp", None), head_spec, head_spec, head_spec, P("tp", None, None),
                P(None, "tp"), P(None, "tp"), P("tp", None), P(None), P(None), act_spec)
    out_specs = (act_spec, act_spec, P("dp", "tp", None), P("dp", "tp", None), P("dp", "tp", None),
                 P(("dp", "tp"), None, None), P("dp", "tp"), P("dp", "tp"), P(("dp", "tp"), None), P("dp"), P("dp"))

    def gather(part):
        return lax.all_gather(part, "tp", axis=0, tiled=True)

    def scatter(part):
        return lax.psum_scatter(part, "tp", scatter_dimension=0, tiled=True)

    def local_step(x_in, positions, w_q, w_k, w_v, w_o, w_gate, w_up, w_down, gain_attn, gain_mlp, d_out):
        n_seq = x_in.shape[0]
        seqs = range(n_seq)
        depth, n_rep, head = w_q.shape
        scale = head ** -0.5
        w_qkv = jnp.concatenate([w.reshape(depth, -1) for w in (w_q, w_k, w_v)], axis=1)
        wo2 = w_o.reshape(-1, depth)
        cos_t, sin_t = rope_tables(positions, head)

        x = [x_in[s] for s in seqs]
        d_y = [d_out[s] for s in seqs]
        latest = []

        def run(fn, first, *rest):
            out = fn(after(first, *latest), *rest)
            latest[:] = jax.tree.leaves(out)[:1]
            return out

        def norm(vals, gain):
            return jax.vjp(rms_norm, vals, gain)

        def mid_norm(proj, vals):
            total = (vals.astype(F32) + proj.astype(F32)).astype(BF)
            return norm(total, gain_mlp) + (total,)

        def mlp_grad(d_g, d_u):
            return rows_times_weights([d_g, d_u], [w_gate, w_up], "nt", 768)

        def down_proj(acts):
            return rows_times_weights([acts], [w_down], "nn", 768)

        def norm_back(cot, pull, skip):
            d_vals, d_gain = pull(cot)
            return skip + d_vals, d_gain

        def add_out(part, vals):
            return (vals.astype(F32) + part.astype(F32)).astype(BF)

        none = [None] * n_seq
        normed_all, attn, attn_part, attn_proj, mlp_all = (list(none) for _ in range(5))
        norm_attn_pull, norm_mlp_pull, mlp_in, hidden, d_act, gated, d_mlp_in = (list(none) for _ in range(7))
        down_out, d_hidden, gain_mlp_part, d_hidden_all, d_qkv, d_normed = (list(none) for _ in range(6))
        grad_x, gain_attn_part, y_out = (list(none) for _ in range(3))

        n_chip = n_tp // 2
        me = lax.axis_index("tp")
        chip, core = me // 2, me % 2
        sibling = [(t, t ^ 1) for t in range(n_tp)]
        onward = [(t, 2 * ((t // 2 + 1 - 2 * (t % 2)) % n_chip) + t % 2) for t in range(n_tp)]
        share = d_out.shape[1]
        back = 2 * core - 1
        offsets = jnp.stack([2 * share * chip, 2 * share * ((chip + back) % n_chip), 2 * share * ((chip - back) % n_chip),
                             2 * share * ((chip + 2) % n_chip) + share * core,
                             2 * share * ((chip + 2) % n_chip) + share * (1 - core)]).astype(jnp.int32)

        def pair_up(mine, other):
            return jnp.where(core == 0, jnp.concatenate([mine, other], axis=1), jnp.concatenate([other, mine], axis=1))

        def own_half(vals):
            return lax.dynamic_slice_in_dim(vals, core * share, share, axis=1)

        dout_sib = lax.ppermute(d_out, "tp", sibling)
        for s in seqs:
            out, norm_attn_pull[s] = run(norm, x[s], gain_attn)
            normed_all[s] = gather(out)
        dout_pair = run(pair_up, d_out, dout_sib)
        dout_near = lax.ppermute(dout_pair, "tp", onward)
        for s in seqs:
            attn[s] = run(attention_fwd, normed_all[s], w_qkv, wo2, cos_t[s], sin_t[s], n_rep, head, scale)
            attn_part[s] = attn[s][4]
        attn_proj[0] = scatter(attn_part[0])
        dout_pass = run(own_half, dout_near)
        dout_far = lax.ppermute(dout_pass, "tp", onward)
        dout_near2 = lax.ppermute(dout_near, "tp", sibling)

        def mid(s):
            mlp_in[s], norm_mlp_pull[s], hidden[s] = run(mid_norm, attn_proj[s], x[s])
            mlp_all[s] = gather(mlp_in[s])

        latest += [dout_far, dout_near2]
        mid(0)
        for s in seqs[1:]:
            attn_proj[s] = scatter(after(attn_part[s], mlp_in[0]))
        dout_far2 = lax.ppermute(after(dout_far, mlp_in[0]), "tp", sibling)
        dout_pieces = (dout_pair, dout_near, dout_near2, dout_far, dout_far2)

        def act_grad(s):
            d_act[s] = run(lambda off: act_cotangent(dout_pieces, off, s, w_down, 512), offsets)

        def mlp_main(s):
            gated[s] = run(gated_mlp, mlp_all[s], w_gate, w_up, d_act[s])

        def mlp_back(s):
            d_mlp_in[s] = scatter(run(mlp_grad, gated[s][1], gated[s][2]))

        def mlp_down(s):
            down_out[s] = scatter(run(down_proj, gated[s][0]))

        def mid_back(s):
            d_hidden[s], gain_mlp_part[s] = run(norm_back, d_mlp_in[s], norm_mlp_pull[s], d_y[s])
            d_hidden_all[s] = gather(d_hidden[s])

        def attn_back(s):
            d_qkv[s], part = run(attention_bwd, d_hidden_all[s], w_qkv, wo2, *attn[s][:3], cos_t[s], sin_t[s], scale)
            d_normed[s] = scatter(part)

        def last_back(s):
            grad_x[s], gain_attn_part[s] = run(norm_back, d_normed[s], norm_attn_pull[s], d_hidden[s])

        act_grad(0)
        mlp_main(0)
        act_grad(1)
        mid(1)
        mlp_back(0)
        mlp_down(0)
        mlp_main(1)
        mid_back(0)
        mlp_back(1)
        mlp_down(1)
        y_out[0] = run(add_out, down_out[0], hidden[0])
        act_out, d_gate, d_up = zip(*gated)
        attn_back(0)
        grad_wdown = run(lambda first: down_grad([first, act_out[1]], dout_pieces, offsets, 768), act_out[0])
        mid_back(1)
        grad_wgate, grad_wup = run(lambda first: weight_grad(
            [first, mlp_all[1]], [d_gate, d_up], (w_gate.shape[1],) * 2, 384, "rows"), mlp_all[0])
        attn_back(1)
        (grad_wo,) = run(lambda first: weight_grad([first, attn[1][3]], [d_hidden_all], (depth,), 768, "cols"),
                         attn[0][3])
        grad_wq, grad_wk, grad_wv = run(lambda first: weight_grad(
            [first, normed_all[1]], [d_qkv], tuple(w[0].size for w in (w_q, w_k, w_v)), 384, "rows"),
            normed_all[0])
        last_back(0)
        y_out[1] = run(add_out, down_out[1], hidden[1])
        last_back(1)
        back_attn, back_mlp = gain_attn_part, gain_mlp_part
        gain_parts = jnp.stack([functools.reduce(jnp.add, back) for back in (back_attn, back_mlp)])
        gains = tp_sum(gain_parts, n_tp)
        return (jnp.stack(y_out), jnp.stack(grad_x), grad_wq.reshape(w_q.shape), grad_wk.reshape(w_k.shape),
                grad_wv.reshape(w_v.shape), grad_wo.reshape(w_o.shape), grad_wgate, grad_wup, grad_wdown,
                gains[0], gains[1])

    return jax.shard_map(local_step, mesh=mesh, in_specs=in_specs, out_specs=out_specs, check_vma=False)
```

```python
import functools

import jax
import jax.numpy as jnp
from jax import lax
from jax.experimental import pallas as pl
from jax.experimental.pallas import tpu as pltpu
from jax.sharding import PartitionSpec as P


EPS = 1e-6
ROPE_THETA = 10000.0
BF = jnp.bfloat16
F32 = jnp.float32
GELU_C = 0.7978845608028654
GELU_A = 0.044715
VMEM_LIMIT = 60 * 1024 * 1024

NN = (((1,), (0,)), ((), ()))
NT = (((1,), (1,)), ((), ()))
TN = (((0,), (0,)), ((), ()))


def rms_norm(vals, gain):
    vals_f32 = vals.astype(F32)
    inv_rms = lax.rsqrt(jnp.mean(vals_f32 * vals_f32, axis=-1, keepdims=True) + EPS)
    return (vals_f32 * inv_rms * (1.0 + gain)).astype(BF)


def rope_tables(positions, head_dim):
    half_dim = head_dim // 2
    inv_freq = ROPE_THETA ** (-2.0 * jnp.arange(half_dim, dtype=F32) / head_dim)
    angles = positions.astype(F32)[:, :, None] * inv_freq
    return jnp.cos(angles), jnp.sin(angles)


def dot(lhs, rhs, dims):
    return lax.dot_general(lhs, rhs, dims, preferred_element_type=F32)


def after(value, *deps):
    return lax.optimization_barrier((value,) + deps)[0]


def join(parts, axis):
    return parts[0] if len(parts) == 1 else jnp.concatenate(parts, axis=axis)


def call(body, grid, in_specs, out_specs, out_shape, flops, nbytes, scratch=()):
    return pl.pallas_call(
        body,
        grid=grid,
        in_specs=in_specs,
        out_specs=out_specs,
        out_shape=out_shape,
        scratch_shapes=scratch,
        compiler_params=pltpu.CompilerParams(vmem_limit_bytes=VMEM_LIMIT),
        cost_estimate=pl.CostEstimate(flops=int(flops), bytes_accessed=int(nbytes), transcendentals=0),
    )


def whole(arr):
    zeros = (0,) * arr.ndim
    return pl.BlockSpec(arr.shape, lambda *_: zeros, pipeline_mode=pl.Buffered(1))


def rows_times_weights(acts, weights, kind, tile, m_tile=256):
    n_rows = acts[0].shape[0]
    nt = kind == "nt"
    n_cols = weights[0].shape[0 if nt else 1]
    depth = sum(a.shape[1] for a in acts)
    n_in = len(acts)
    grid = (pl.cdiv(n_cols, tile),)

    def body(*refs):
        a_refs, w_refs, out = refs[:n_in], refs[n_in:-1], refs[-1]
        rhs = join([w[...] for w in w_refs], 1 if nt else 0)
        for start in range(0, n_rows, m_tile):
            rows = pl.ds(start, m_tile)
            lhs = join([a[rows, :] for a in a_refs], 1)
            out[rows, :] = dot(lhs, rhs, NT if nt else NN).astype(BF)

    if nt:
        w_specs = [pl.BlockSpec((tile, w.shape[1]), lambda i: (i, 0)) for w in weights]
    else:
        w_specs = [pl.BlockSpec((w.shape[0], tile), lambda i: (0, i)) for w in weights]
    return call(
        body, grid, [whole(a) for a in acts] + w_specs,
        pl.BlockSpec((n_rows, tile), lambda i: (0, i)),
        jax.ShapeDtypeStruct((n_rows, n_cols), BF),
        2 * n_rows * depth * n_cols, 2 * (n_rows * depth + depth * n_cols + n_rows * n_cols),
    )(*acts, *weights)


def rotate(vals, cos_t, sin_t):
    half = cos_t.shape[1]
    first, second = vals[:, :half].astype(F32), vals[:, half:].astype(F32)
    return jnp.concatenate([first * cos_t - second * sin_t, second * cos_t + first * sin_t], axis=1)


def unrotate(vals, cos_t, sin_t):
    half = cos_t.shape[1]
    first, second = vals[:, :half], vals[:, half:]
    return jnp.concatenate([first * cos_t + second * sin_t, second * cos_t - first * sin_t], axis=1)


def causal_probs(q_rows, k_rot, start, tile, n_rep):
    end = start + tile
    scores = dot(q_rows, k_rot[:end], NT)
    row = lax.broadcasted_iota(jnp.int32, (n_rep * tile, end), 0)
    col = lax.broadcasted_iota(jnp.int32, (n_rep * tile, end), 1)
    scores = jnp.where(lax.rem(row, tile) + start >= col, scores, -1e30)
    probs = jnp.exp(scores - jnp.max(scores, axis=1, keepdims=True))
    return probs / jnp.sum(probs, axis=1, keepdims=True)


def attention_fwd(acts, w_qkv, w_o, cos_t, sin_t, n_rep, head, scale):
    n_rows, depth = acts.shape
    n_q, width = n_rep * head, w_qkv.shape[1]
    tile = 256
    n_tiles, n_cols = n_rows // tile, width // tile

    def body(acts_hbm, w_hbm, wo_hbm, cos_ref, sin_ref, q_rot, k_rot, v, out, part_hbm,
             acts_v, w_v, wo_v, qkv, part_v, a_sem, w_sem, wo_sem, o_sem):
        a_copy = [pltpu.make_async_copy(acts_hbm.at[pl.ds(i * tile, tile)], acts_v.at[pl.ds(i * tile, tile)],
                                        a_sem.at[i]) for i in range(n_tiles)]
        w_copy = [pltpu.make_async_copy(w_hbm.at[:, pl.ds(i * tile, tile)], w_v.at[:, pl.ds(i * tile, tile)],
                                        w_sem.at[i]) for i in range(n_cols)]
        wo_copy = pltpu.make_async_copy(wo_hbm, wo_v, wo_sem)
        o_copy = [pltpu.make_async_copy(part_v.at[i % 2], part_hbm.at[pl.ds(i * tile, tile)], o_sem.at[i % 2])
                  for i in range(n_tiles)]
        for copy in a_copy[:1] + w_copy + [wo_copy] + a_copy[1:]:
            copy.start()
        for i in range(n_tiles):
            rows = pl.ds(i * tile, tile)
            a_copy[i].wait()
            if i == 0:
                for j in range(n_cols):
                    w_copy[j].wait()
                    cols = pl.ds(j * tile, tile)
                    qkv[:, cols] = dot(acts_v[rows, :], w_v[:, cols], NN).astype(BF)
                wo_copy.wait()
            else:
                qkv[...] = dot(acts_v[rows, :], w_v[...], NN).astype(BF)
            cos, sin = cos_ref[rows, :], sin_ref[rows, :]
            k_rot[rows, :] = rotate(qkv[:, n_q:n_q + head], cos, sin).astype(BF)
            v[rows, :] = qkv[:, n_q + head:]
            q_rows = join([(rotate(qkv[:, h * head:(h + 1) * head], cos, sin) * scale).astype(BF)
                           for h in range(n_rep)], 0)
            probs = causal_probs(q_rows, k_rot, i * tile, tile, n_rep).astype(BF)
            mixed = dot(probs, v[: (i + 1) * tile], NN).astype(BF)
            for h in range(n_rep):
                cols = pl.ds(h * head, head)
                q_rot[rows, cols] = q_rows[h * tile:(h + 1) * tile]
                out[rows, cols] = mixed[h * tile:(h + 1) * tile]
            if i >= 2:
                o_copy[i].wait()
            heads = join([mixed[h * tile:(h + 1) * tile] for h in range(n_rep)], 1)
            part_v[i % 2] = dot(heads, wo_v[...], NN).astype(BF)
            o_copy[i].start()
        for i in range(max(0, n_tiles - 2), n_tiles):
            o_copy[i].wait()

    any_spec = pl.BlockSpec(memory_space=pl.ANY)
    outs = [jax.ShapeDtypeStruct((n_rows, w), BF) for w in (n_q, head, head, n_q)]
    return call(
        body, (1,), [any_spec] * 3 + [whole(cos_t), whole(sin_t)], [whole(o) for o in outs] + [any_spec],
        outs + [jax.ShapeDtypeStruct((n_rows, depth), BF)],
        2 * n_rows * depth * (width + n_q) + 4e9, 2 * (2 * n_rows * depth + depth * (width + n_q)),
        [pltpu.VMEM((n_rows, depth), BF), pltpu.VMEM(w_qkv.shape, BF), pltpu.VMEM(w_o.shape, BF),
         pltpu.VMEM((tile, width), BF), pltpu.VMEM((2, tile, depth), BF),
         pltpu.SemaphoreType.DMA((n_tiles,)), pltpu.SemaphoreType.DMA((n_cols,)), pltpu.SemaphoreType.DMA,
         pltpu.SemaphoreType.DMA((2,))],
    )(acts, w_qkv, w_o, cos_t, sin_t)


def attention_bwd(cot, w_qkv, w_o, q_rot, k_rot, v_raw, cos_t, sin_t, scale):
    n_rows, depth = cot.shape
    head = k_rot.shape[1]
    n_q, width = q_rot.shape[1], w_qkv.shape[1]
    n_rep = n_q // head
    tile = 256
    n_tiles = n_rows // tile

    def body(cot_hbm, w_hbm, wo_hbm, q, k, v, cos_ref, sin_ref, d_qkv, part_hbm,
             cot_v, w_v, wo_v, part_v, dk_acc, dv_acc, c_sem, w_sem, wo_sem, o_sem):
        order = list(reversed(range(n_tiles)))
        c_copy = [pltpu.make_async_copy(cot_hbm.at[pl.ds(i * tile, tile)], cot_v.at[pl.ds(i * tile, tile)],
                                        c_sem.at[i]) for i in range(n_tiles)]
        w_copy = pltpu.make_async_copy(w_hbm, w_v, w_sem)
        wo_copy = pltpu.make_async_copy(wo_hbm, wo_v, wo_sem)
        o_copy = [pltpu.make_async_copy(part_v.at[i % 2], part_hbm.at[pl.ds(i * tile, tile)], o_sem.at[i % 2])
                  for i in range(n_tiles)]
        for copy in [wo_copy] + [c_copy[i] for i in order[:1]] + [w_copy] + [c_copy[i] for i in order[1:]]:
            copy.start()
        wo_copy.wait()
        for n, i in enumerate(order):
            rows, end = pl.ds(i * tile, tile), (i + 1) * tile
            c_copy[i].wait()
            d_o = dot(cot_v[rows, :], wo_v[...], NT).astype(BF)
            q_rows = join([q[rows, pl.ds(h * head, head)] for h in range(n_rep)], 0)
            do_rows = join([d_o[:, h * head:(h + 1) * head] for h in range(n_rep)], 0)
            probs = causal_probs(q_rows, k, i * tile, tile, n_rep)
            d_probs = dot(do_rows, v[:end], NT)
            d_scores = (probs * (d_probs - jnp.sum(d_probs * probs, axis=1, keepdims=True))).astype(BF)
            dv_part = dot(probs.astype(BF), do_rows, TN)
            dk_part = dot(d_scores, q_rows, TN)
            if n == 0:
                dv_acc[...] = dv_part
                dk_acc[...] = dk_part
            else:
                dv_acc[:end] += dv_part
                dk_acc[:end] += dk_part
            dq_rows = dot(d_scores, k[:end], NN).astype(BF).astype(F32) * scale
            cos, sin = cos_ref[rows, :], sin_ref[rows, :]
            parts = [unrotate(dq_rows[h * tile:(h + 1) * tile], cos, sin).astype(BF) for h in range(n_rep)]
            parts.append(unrotate(dk_acc[rows, :].astype(BF).astype(F32), cos, sin).astype(BF))
            parts.append(dv_acc[rows, :].astype(BF))
            tile_grad = join(parts, 1)
            d_qkv[rows, :] = tile_grad
            if n == 0:
                w_copy.wait()
            if n >= 2:
                o_copy[i].wait()
            part_v[i % 2] = dot(tile_grad, w_v[...], NT).astype(BF)
            o_copy[i].start()
        for i in order[-2:]:
            o_copy[i].wait()

    any_spec = pl.BlockSpec(memory_space=pl.ANY)
    rest = (q_rot, k_rot, v_raw, cos_t, sin_t)
    outs = [jax.ShapeDtypeStruct((n_rows, width), BF), jax.ShapeDtypeStruct((n_rows, depth), BF)]
    return call(
        body, (1,), [any_spec] * 3 + [whole(r) for r in rest], [whole(outs[0]), any_spec], outs,
        2 * n_rows * depth * (width + n_q) + 8e9, 2 * (2 * n_rows * depth + depth * (width + n_q)),
        [pltpu.VMEM((n_rows, depth), BF), pltpu.VMEM(w_qkv.shape, BF), pltpu.VMEM(w_o.shape, BF),
         pltpu.VMEM((2, tile, depth), BF), pltpu.VMEM((n_rows, head), F32), pltpu.VMEM((n_rows, head), F32),
         pltpu.SemaphoreType.DMA((n_tiles,)), pltpu.SemaphoreType.DMA, pltpu.SemaphoreType.DMA,
         pltpu.SemaphoreType.DMA((2,))],
    )(cot, w_qkv, w_o, *rest)


def aligned(offset):
    return pl.multiple_of(offset, 128)


def act_cotangent(pieces, offsets, seq, w_down, gate, up, tile):
    width, depth = w_down.shape
    n_rows = sum(p.shape[1] for p in pieces)
    n_pieces = len(pieces)

    def body(off_ref, *refs):
        p_refs, (w_ref, g_ref, u_ref, dg_ref, du_ref) = refs[:n_pieces], refs[n_pieces:]
        rhs = w_ref[...]
        for group in ([0], [1], [2], [3, 4]):
            vals = dot(join([p_refs[g][...] for g in group], 0), rhs, NT).astype(BF)
            at = 0
            for g in group:
                size = p_refs[g].shape[0]
                rows = pl.ds(aligned(off_ref[g]), size)
                d_z = vals[at:at + size].astype(F32)
                at += size
                gate_v, up_v = g_ref[rows, :].astype(F32), u_ref[rows, :].astype(F32)
                square = gate_v * gate_v
                tanh = jnp.tanh(gate_v * (GELU_C + (GELU_C * GELU_A) * square))
                half = 0.5 + 0.5 * tanh
                slope = half + (0.5 * gate_v) * (1.0 - tanh * tanh) * (GELU_C + (3.0 * GELU_C * GELU_A) * square)
                du_ref[rows, :] = (d_z * (gate_v * half)).astype(BF)
                dg_ref[rows, :] = (d_z * up_v * slope).astype(BF)

    p_specs = [pl.BlockSpec((None,) + p.shape[1:], lambda i: (seq, 0, 0), pipeline_mode=pl.Buffered(1)) for p in pieces]
    o_spec = pl.BlockSpec((n_rows, tile), lambda i: (0, i))
    return call(
        body, (pl.cdiv(width, tile),),
        [pl.BlockSpec(memory_space=pltpu.SMEM)] + p_specs + [pl.BlockSpec((tile, depth), lambda i: (i, 0)), o_spec, o_spec],
        [o_spec] * 2, [jax.ShapeDtypeStruct((n_rows, width), BF)] * 2,
        2 * n_rows * depth * width, 2 * (n_rows * depth + depth * width + 4 * n_rows * width),
    )(offsets, *pieces, w_down, gate, up)


def down_grad(acts, pieces, offsets, tile):
    n_seq = len(acts)
    n_tok, width = acts[0].shape
    depth = pieces[0].shape[2]

    def body(off_ref, *refs):
        z_refs, p_refs, out = refs[:n_seq], refs[n_seq:-1], refs[-1]
        left = join([z[pl.ds(aligned(off_ref[g]), p.shape[1]), :] for z in z_refs for g, p in enumerate(p_refs)], 0)
        right = join([p[s] for s in range(n_seq) for p in p_refs], 0)
        out[...] = dot(left, right, TN).astype(BF)

    p_specs = [pl.BlockSpec(p.shape[:2] + (tile,), lambda i: (0, 0, i)) for p in pieces]
    return call(
        body, (depth // tile,),
        [pl.BlockSpec(memory_space=pltpu.SMEM)] + [whole(z) for z in acts] + p_specs,
        pl.BlockSpec((width, tile), lambda i: (0, i)), jax.ShapeDtypeStruct((width, depth), BF),
        2 * n_seq * n_tok * width * depth, 2 * (n_seq * n_tok * (width + depth) + width * depth),
    )(offsets, *acts, *pieces)


def gated_mlp(acts, w_gate, w_up):
    n_rows, depth = acts.shape
    width = w_gate.shape[1]
    tile, m_tile = 384, 256

    def body(a_ref, wg, wu, g_ref, u_ref, z_ref):
        rhs = jnp.concatenate([wg[...], wu[...]], axis=1)
        for start in range(0, n_rows, m_tile):
            rows = pl.ds(start, m_tile)
            both = dot(a_ref[rows, :], rhs, NN).astype(BF)
            g_ref[rows, :] = both[:, :tile]
            u_ref[rows, :] = both[:, tile:]
            gate = both[:, :tile].astype(F32)
            half = 0.5 + 0.5 * jnp.tanh(gate * (GELU_C + (GELU_C * GELU_A) * (gate * gate)))
            z_ref[rows, :] = (gate * half * both[:, tile:].astype(F32)).astype(BF)

    w_spec = pl.BlockSpec((depth, tile), lambda i: (0, i))
    o_spec = pl.BlockSpec((n_rows, tile), lambda i: (0, i))
    return call(
        body, (width // tile,), [whole(acts), w_spec, w_spec], [o_spec] * 3,
        [jax.ShapeDtypeStruct((n_rows, width), BF)] * 3,
        4 * n_rows * depth * width, 2 * (n_rows * depth + 2 * depth * width + 3 * n_rows * width),
    )(acts, w_gate, w_up)


def down_proj(acts, w_down, starts, tile):
    n_rows, width = acts.shape
    depth = w_down.shape[1]
    half, part = n_rows // 2, n_rows // 8

    def body(off_ref, z_ref, w_ref, keep, give):
        rhs = w_ref[...]

        def rows(n, size):
            return z_ref[pl.ds(aligned(off_ref[n]), size), :]

        for base, out in ((0, keep), (3, give)):
            out[:2 * part] = dot(rows(base, 2 * part), rhs, NN).astype(BF)
            out[2 * part:] = dot(join([rows(base + 1, part), rows(base + 2, part)], 0), rhs, NN).astype(BF)

    o_spec = pl.BlockSpec((half, tile), lambda i: (0, i))
    return call(
        body, (depth // tile,),
        [pl.BlockSpec(memory_space=pltpu.SMEM), whole(acts), pl.BlockSpec((width, tile), lambda i: (0, i))],
        [o_spec] * 2, [jax.ShapeDtypeStruct((half, depth), BF)] * 2,
        2 * n_rows * depth * width, 2 * (n_rows * width + depth * width + n_rows * depth),
    )(starts, acts, w_down)


def weight_grad(lhs, rhs_groups, out_widths, tile, stream):
    n_seq, n_tok = len(lhs), lhs[0].shape[0]
    n_out = lhs[0].shape[1]
    rhs = [r for group in rhs_groups for r in group]
    n_groups = len(rhs_groups)

    def body(*refs):
        l_refs, r_refs, o_refs = refs[:n_seq], refs[n_seq:n_seq + n_seq * n_groups], refs[n_seq + n_seq * n_groups:]
        left = join([l[...] for l in l_refs], 0)
        right = join([join([r_refs[g * n_seq + s][...] for s in range(n_seq)], 0) for g in range(n_groups)], 1)
        acc = dot(left, right, TN)
        at = 0
        for o in o_refs:
            o[...] = acc[:, at:at + o.shape[1]].astype(BF)
            at += o.shape[1]

    if stream == "rows":
        grid = (n_out // tile,)
        l_specs = [pl.BlockSpec((n_tok, tile), lambda i: (0, i)) for _ in lhs]
        r_specs = [whole(r) for r in rhs]
        o_specs = [pl.BlockSpec((tile, w), lambda i: (i, 0)) for w in out_widths]
    else:
        grid = (out_widths[0] // tile,)
        l_specs = [whole(l) for l in lhs]
        r_specs = [pl.BlockSpec((n_tok, tile), lambda i: (0, i)) for _ in rhs]
        o_specs = [pl.BlockSpec((n_out, tile), lambda i: (0, i)) for _ in out_widths]
    total = sum(out_widths)
    return call(
        body, grid, l_specs + r_specs, o_specs,
        [jax.ShapeDtypeStruct((n_out, w), BF) for w in out_widths],
        2 * n_seq * n_tok * n_out * total, 2 * (n_seq * n_tok * (n_out + total) + n_out * total),
    )(*lhs, *rhs)


def tp_sum(part, n_tp):
    def body(x_ref, out_ref, slots, send_sem, recv_sem):
        me = lax.axis_index("tp")
        barrier = pltpu.get_barrier_semaphore()
        for step in range(1, n_tp):
            pl.semaphore_signal(barrier, inc=1, device_id={"tp": lax.rem(me + step, n_tp)},
                                device_id_type=pl.DeviceIdType.MESH)
        pl.semaphore_wait(barrier, n_tp - 1)
        copies = []
        for step in range(1, n_tp):
            copies.append(pltpu.make_async_remote_copy(
                src_ref=x_ref, dst_ref=slots.at[me], send_sem=send_sem.at[step], recv_sem=recv_sem.at[step],
                device_id={"tp": lax.rem(me + step, n_tp)}, device_id_type=pl.DeviceIdType.MESH))
            copies[-1].start()
        slots[me] = x_ref[...]
        for copy in copies:
            copy.wait()
        total = slots[0]
        for step in range(1, n_tp):
            total = total + slots[step]
        out_ref[...] = total

    return pl.pallas_call(
        body,
        out_shape=jax.ShapeDtypeStruct(part.shape, F32),
        in_specs=[pl.BlockSpec(memory_space=pltpu.VMEM)],
        out_specs=pl.BlockSpec(memory_space=pltpu.VMEM),
        scratch_shapes=[pltpu.VMEM((n_tp,) + part.shape, F32), pltpu.SemaphoreType.DMA((n_tp,)),
                        pltpu.SemaphoreType.DMA((n_tp,))],
        compiler_params=pltpu.CompilerParams(collective_id=0, has_side_effects=True),
        cost_estimate=pl.CostEstimate(flops=5_000_000_000, bytes_accessed=1_000_000, transcendentals=0),
        name="tp_sum",
    )(part)


def solution(mesh):
    n_tp = mesh.shape["tp"]
    act_spec = P("dp", "tp", None)
    head_spec = P(None, "tp", None)
    in_specs = (act_spec, P("dp", None), head_spec, head_spec, head_spec, P("tp", None, None),
                P(None, "tp"), P(None, "tp"), P("tp", None), P(None), P(None), act_spec)
    out_specs = (act_spec, act_spec, P("dp", "tp", None), P("dp", "tp", None), P("dp", "tp", None),
                 P(("dp", "tp"), None, None), P("dp", "tp"), P("dp", "tp"), P(("dp", "tp"), None), P("dp"), P("dp"))

    def gather(part):
        return lax.all_gather(part, "tp", axis=0, tiled=True)

    def scatter(part):
        return lax.psum_scatter(part, "tp", scatter_dimension=0, tiled=True)

    def local_step(x_in, positions, w_q, w_k, w_v, w_o, w_gate, w_up, w_down, gain_attn, gain_mlp, d_out):
        n_seq = x_in.shape[0]
        seqs = range(n_seq)
        depth, n_rep, head = w_q.shape
        scale = head ** -0.5
        w_qkv = jnp.concatenate([w.reshape(depth, -1) for w in (w_q, w_k, w_v)], axis=1)
        wo2 = w_o.reshape(-1, depth)
        cos_t, sin_t = rope_tables(positions, head)

        x = [x_in[s] for s in seqs]
        d_y = [d_out[s] for s in seqs]
        latest = []

        def run(fn, first, *rest):
            out = fn(after(first, *latest), *rest)
            latest[:] = jax.tree.leaves(out)[:1]
            return out

        def norm(vals, gain):
            return jax.vjp(rms_norm, vals, gain)

        def mid_norm(proj, vals):
            total = (vals.astype(F32) + proj.astype(F32)).astype(BF)
            return norm(total, gain_mlp) + (total,)

        def mlp_grad(d_g, d_u):
            return rows_times_weights([d_g, d_u], [w_gate, w_up], "nt", 768)

        def norm_back(cot, pull, skip):
            d_vals, d_gain = pull(cot)
            return skip + d_vals, d_gain

        none = [None] * n_seq
        normed_all, attn, attn_part, attn_proj, mlp_all = (list(none) for _ in range(5))
        norm_attn_pull, norm_mlp_pull, mlp_in, hidden, _, gated, d_mlp_in = (list(none) for _ in range(7))
        _, d_hidden, gain_mlp_part, d_hidden_all, d_qkv, d_normed = (list(none) for _ in range(6))
        grad_x, gain_attn_part = (list(none) for _ in range(2))

        n_chip = n_tp // 2
        me = lax.axis_index("tp")
        chip, core = me // 2, me % 2
        sibling = [(t, t ^ 1) for t in range(n_tp)]
        onward = [(t, 2 * ((t // 2 + 1 - 2 * (t % 2)) % n_chip) + t % 2) for t in range(n_tp)]
        share = d_out.shape[1]
        back = 2 * core - 1
        offsets = jnp.stack([2 * share * chip, 2 * share * ((chip + back) % n_chip), 2 * share * ((chip - back) % n_chip),
                             2 * share * ((chip + 2) % n_chip) + share * core,
                             2 * share * ((chip + 2) % n_chip) + share * (1 - core)]).astype(jnp.int32)

        def pair_up(mine, other):
            return jnp.where(core == 0, jnp.concatenate([mine, other], axis=1), jnp.concatenate([other, mine], axis=1))

        def own_half(vals):
            return lax.dynamic_slice_in_dim(vals, core * share, share, axis=1)

        keeps = jnp.stack([2 * share * ((chip - back) % n_chip), 2 * share * ((chip + 2) % n_chip) + share * core,
                           2 * share * chip + share * core, 2 * share * ((chip + back) % n_chip),
                           2 * share * ((chip + 2) % n_chip) + share * (1 - core),
                           2 * share * chip + share * (1 - core)]).astype(jnp.int32)

        dout_sib = lax.ppermute(d_out, "tp", sibling)
        for s in seqs:
            out, norm_attn_pull[s] = run(norm, x[s], gain_attn)
            normed_all[s] = gather(out)
        dout_pair = run(pair_up, d_out, dout_sib)
        for s in seqs:
            attn[s] = run(attention_fwd, normed_all[s], w_qkv, wo2, cos_t[s], sin_t[s], n_rep, head, scale)
            attn_part[s] = attn[s][4]
        attn_proj[0] = scatter(attn_part[0])
        dout_near = lax.ppermute(after(dout_pair, attn_part[1]), "tp", onward)

        def mid(s):
            mlp_in[s], norm_mlp_pull[s], hidden[s] = run(mid_norm, attn_proj[s], x[s])
            mlp_all[s] = gather(mlp_in[s])

        def mlp_main(s):
            gated[s] = run(gated_mlp, mlp_all[s], w_gate, w_up)

        def mlp_down(s):
            keep, give = run(lambda z: down_proj(z, w_down, keeps, 768), gated[s][2])
            down_keep[s] = keep
            down_got[s] = lax.ppermute(give, "tp", sibling)

        down_keep, down_got, d_gate, d_up = (list(none) for _ in range(4))
        mid(0)
        for s in seqs[1:]:
            attn_proj[s] = scatter(after(attn_part[s], mlp_in[0]))
        dout_pass = run(own_half, dout_near)
        dout_far = lax.ppermute(dout_pass, "tp", onward)
        dout_near2 = lax.ppermute(after(dout_near, dout_pass), "tp", sibling)
        mlp_main(0)
        dout_far2 = lax.ppermute(after(dout_far, *latest), "tp", sibling)
        mlp_down(0)
        dout_pieces = (dout_pair, dout_near, dout_near2, dout_far, dout_far2)
        mid(1)

        def act_grad(s):
            d_gate[s], d_up[s] = run(lambda off: act_cotangent(dout_pieces, off, s, w_down, *gated[s][:2], 512), offsets)

        def mlp_back(s):
            d_mlp_in[s] = scatter(run(mlp_grad, d_gate[s], d_up[s]))

        def mid_back(s):
            d_hidden[s], gain_mlp_part[s] = run(norm_back, d_mlp_in[s], norm_mlp_pull[s], d_y[s])
            d_hidden_all[s] = gather(d_hidden[s])

        def attn_back(s):
            d_qkv[s], part = run(attention_bwd, d_hidden_all[s], w_qkv, wo2, *attn[s][:3], cos_t[s], sin_t[s], scale)
            d_normed[s] = scatter(part)

        def last_back(s):
            grad_x[s], gain_attn_part[s] = run(norm_back, d_normed[s], norm_attn_pull[s], d_hidden[s])

        def halves(keep0, keep1, got0, got1):
            total = jnp.stack([(k.astype(F32) + g.astype(F32)).astype(BF) for k, g in ((keep0, got0), (keep1, got1))])
            return total[:, 2 * share:3 * share], total[:, :2 * share], total[:, 3 * share:]

        def pass_on(near, far):
            row = lax.broadcasted_iota(jnp.int32, (1, 2 * share, 1), 1) // share
            both = jnp.concatenate([far, far], axis=1).astype(F32)
            return (near.astype(F32) + jnp.where(row == core, both, 0.0)).astype(BF)

        def own_rows(vals):
            return own_half(vals), lax.dynamic_slice_in_dim(vals, (1 - core) * share, share, axis=1)

        def finish(mine, near, other):
            total = (mine.astype(F32) + near.astype(F32) + other.astype(F32)).astype(BF)
            return (jnp.stack(hidden).astype(F32) + total.astype(F32)).astype(BF)

        act_grad(0)
        mlp_back(0)
        mlp_main(1)
        act_grad(1)
        mid_back(0)
        mlp_back(1)
        mlp_down(1)
        attn_back(0)
        down_far, down_near, down_own = run(halves, down_keep[0], down_keep[1], *down_got)
        far_in = lax.ppermute(down_far, "tp", onward)
        mid_back(1)
        act_out = [g[2] for g in gated]
        grad_wgate, grad_wup = run(lambda first: weight_grad(
            [first, mlp_all[1]], [d_gate, d_up], (w_gate.shape[1],) * 2, 384, "rows"), mlp_all[0])
        down_near = run(pass_on, down_near, far_in)
        near_in = lax.ppermute(down_near, "tp", onward)
        grad_wdown = run(lambda first: down_grad([first, act_out[1]], dout_pieces, offsets, 768), act_out[0])
        attn_back(1)
        near_mine, near_other = run(own_rows, near_in)
        other_in = lax.ppermute(near_other, "tp", sibling)
        (grad_wo,) = run(lambda first: weight_grad([first, attn[1][3]], [d_hidden_all], (depth,), 768, "cols"),
                         attn[0][3])
        grad_wq, grad_wk, grad_wv = run(lambda first: weight_grad(
            [first, normed_all[1]], [d_qkv], tuple(w[0].size for w in (w_q, w_k, w_v)), 384, "rows"),
            normed_all[0])
        y_out = run(finish, down_own, near_mine, other_in)
        last_back(0)
        last_back(1)
        back_attn, back_mlp = gain_attn_part, gain_mlp_part
        gain_parts = jnp.stack([functools.reduce(jnp.add, back) for back in (back_attn, back_mlp)])
        gains = tp_sum(gain_parts, n_tp)
        return (y_out, jnp.stack(grad_x), grad_wq.reshape(w_q.shape), grad_wk.reshape(w_k.shape),
                grad_wv.reshape(w_v.shape), grad_wo.reshape(w_o.shape), grad_wgate, grad_wup, grad_wdown,
                gains[0], gains[1])

    return jax.shard_map(local_step, mesh=mesh, in_specs=in_specs, out_specs=out_specs, check_vma=False)
```

```python
import functools

import jax
import jax.numpy as jnp
from jax import lax
from jax.experimental import pallas as pl
from jax.experimental.pallas import tpu as pltpu
from jax.sharding import PartitionSpec as P


EPS = 1e-6
ROPE_THETA = 10000.0
BF = jnp.bfloat16
F32 = jnp.float32
GELU_C = 0.7978845608028654
GELU_A = 0.044715
VMEM_LIMIT = 60 * 1024 * 1024

NN = (((1,), (0,)), ((), ()))
NT = (((1,), (1,)), ((), ()))
TN = (((0,), (0,)), ((), ()))


def rms_norm(vals, gain):
    vals_f32 = vals.astype(F32)
    inv_rms = lax.rsqrt(jnp.mean(vals_f32 * vals_f32, axis=-1, keepdims=True) + EPS)
    return (vals_f32 * inv_rms * (1.0 + gain)).astype(BF)


def rope_tables(positions, head_dim):
    half_dim = head_dim // 2
    inv_freq = ROPE_THETA ** (-2.0 * jnp.arange(half_dim, dtype=F32) / head_dim)
    angles = positions.astype(F32)[:, :, None] * inv_freq
    return jnp.cos(angles), jnp.sin(angles)


def dot(lhs, rhs, dims):
    return lax.dot_general(lhs, rhs, dims, preferred_element_type=F32)


def after(value, *deps):
    return lax.optimization_barrier((value,) + deps)[0]


def join(parts, axis):
    return parts[0] if len(parts) == 1 else jnp.concatenate(parts, axis=axis)


def call(body, grid, in_specs, out_specs, out_shape, flops, nbytes, scratch=()):
    return pl.pallas_call(
        body,
        grid=grid,
        in_specs=in_specs,
        out_specs=out_specs,
        out_shape=out_shape,
        scratch_shapes=scratch,
        compiler_params=pltpu.CompilerParams(vmem_limit_bytes=VMEM_LIMIT),
        cost_estimate=pl.CostEstimate(flops=int(flops), bytes_accessed=int(nbytes), transcendentals=0),
    )


def whole(arr):
    zeros = (0,) * arr.ndim
    return pl.BlockSpec(arr.shape, lambda *_: zeros, pipeline_mode=pl.Buffered(1))


def rows_times_weights(acts, weights, kind, tile, m_tile=256):
    n_rows = acts[0].shape[0]
    nt = kind == "nt"
    n_cols = weights[0].shape[0 if nt else 1]
    depth = sum(a.shape[1] for a in acts)
    n_in = len(acts)
    grid = (pl.cdiv(n_cols, tile),)

    def body(*refs):
        a_refs, w_refs, out = refs[:n_in], refs[n_in:-1], refs[-1]
        rhs = join([w[...] for w in w_refs], 1 if nt else 0)
        for start in range(0, n_rows, m_tile):
            rows = pl.ds(start, m_tile)
            lhs = join([a[rows, :] for a in a_refs], 1)
            out[rows, :] = dot(lhs, rhs, NT if nt else NN).astype(BF)

    if nt:
        w_specs = [pl.BlockSpec((tile, w.shape[1]), lambda i: (i, 0)) for w in weights]
    else:
        w_specs = [pl.BlockSpec((w.shape[0], tile), lambda i: (0, i)) for w in weights]
    return call(
        body, grid, [whole(a) for a in acts] + w_specs,
        pl.BlockSpec((n_rows, tile), lambda i: (0, i)),
        jax.ShapeDtypeStruct((n_rows, n_cols), BF),
        2 * n_rows * depth * n_cols, 2 * (n_rows * depth + depth * n_cols + n_rows * n_cols),
    )(*acts, *weights)


def rotate(vals, cos_t, sin_t):
    half = cos_t.shape[1]
    first, second = vals[:, :half].astype(F32), vals[:, half:].astype(F32)
    return jnp.concatenate([first * cos_t - second * sin_t, second * cos_t + first * sin_t], axis=1)


def unrotate(vals, cos_t, sin_t):
    half = cos_t.shape[1]
    first, second = vals[:, :half], vals[:, half:]
    return jnp.concatenate([first * cos_t + second * sin_t, second * cos_t - first * sin_t], axis=1)


def causal_probs(q_rows, k_rot, start, tile, n_rep):
    end = start + tile
    scores = dot(q_rows, k_rot[:end], NT)
    row = lax.broadcasted_iota(jnp.int32, (n_rep * tile, end), 0)
    col = lax.broadcasted_iota(jnp.int32, (n_rep * tile, end), 1)
    scores = jnp.where(lax.rem(row, tile) + start >= col, scores, -1e30)
    probs = jnp.exp(scores - jnp.max(scores, axis=1, keepdims=True))
    return probs / jnp.sum(probs, axis=1, keepdims=True)


def attention_fwd(acts, w_qkv, w_o, cos_t, sin_t, n_rep, head, scale):
    n_rows, depth = acts.shape
    n_q, width = n_rep * head, w_qkv.shape[1]
    tile = 256
    n_tiles, n_cols = n_rows // tile, width // tile

    def body(acts_hbm, w_hbm, wo_hbm, cos_ref, sin_ref, q_rot, k_rot, v, out, part_hbm,
             acts_v, w_v, wo_v, qkv, part_v, a_sem, w_sem, wo_sem, o_sem):
        a_copy = [pltpu.make_async_copy(acts_hbm.at[pl.ds(i * tile, tile)], acts_v.at[pl.ds(i * tile, tile)],
                                        a_sem.at[i]) for i in range(n_tiles)]
        w_copy = [pltpu.make_async_copy(w_hbm.at[:, pl.ds(i * tile, tile)], w_v.at[:, pl.ds(i * tile, tile)],
                                        w_sem.at[i]) for i in range(n_cols)]
        wo_copy = pltpu.make_async_copy(wo_hbm, wo_v, wo_sem)
        o_copy = [pltpu.make_async_copy(part_v.at[i % 2], part_hbm.at[pl.ds(i * tile, tile)], o_sem.at[i % 2])
                  for i in range(n_tiles)]
        for copy in a_copy[:1] + w_copy + [wo_copy] + a_copy[1:]:
            copy.start()
        for i in range(n_tiles):
            rows = pl.ds(i * tile, tile)
            a_copy[i].wait()
            if i == 0:
                for j in range(n_cols):
                    w_copy[j].wait()
                    cols = pl.ds(j * tile, tile)
                    qkv[:, cols] = dot(acts_v[rows, :], w_v[:, cols], NN).astype(BF)
                wo_copy.wait()
            else:
                qkv[...] = dot(acts_v[rows, :], w_v[...], NN).astype(BF)
            cos, sin = cos_ref[rows, :], sin_ref[rows, :]
            k_rot[rows, :] = rotate(qkv[:, n_q:n_q + head], cos, sin).astype(BF)
            v[rows, :] = qkv[:, n_q + head:]
            q_rows = join([(rotate(qkv[:, h * head:(h + 1) * head], cos, sin) * scale).astype(BF)
                           for h in range(n_rep)], 0)
            probs = causal_probs(q_rows, k_rot, i * tile, tile, n_rep).astype(BF)
            mixed = dot(probs, v[: (i + 1) * tile], NN).astype(BF)
            for h in range(n_rep):
                cols = pl.ds(h * head, head)
                q_rot[rows, cols] = q_rows[h * tile:(h + 1) * tile]
                out[rows, cols] = mixed[h * tile:(h + 1) * tile]
            if i >= 2:
                o_copy[i].wait()
            heads = join([mixed[h * tile:(h + 1) * tile] for h in range(n_rep)], 1)
            part_v[i % 2] = dot(heads, wo_v[...], NN).astype(BF)
            o_copy[i].start()
        for i in range(max(0, n_tiles - 2), n_tiles):
            o_copy[i].wait()

    any_spec = pl.BlockSpec(memory_space=pl.ANY)
    outs = [jax.ShapeDtypeStruct((n_rows, w), BF) for w in (n_q, head, head, n_q)]
    return call(
        body, (1,), [any_spec] * 3 + [whole(cos_t), whole(sin_t)], [whole(o) for o in outs] + [any_spec],
        outs + [jax.ShapeDtypeStruct((n_rows, depth), BF)],
        2 * n_rows * depth * (width + n_q) + 4e9, 2 * (2 * n_rows * depth + depth * (width + n_q)),
        [pltpu.VMEM((n_rows, depth), BF), pltpu.VMEM(w_qkv.shape, BF), pltpu.VMEM(w_o.shape, BF),
         pltpu.VMEM((tile, width), BF), pltpu.VMEM((2, tile, depth), BF),
         pltpu.SemaphoreType.DMA((n_tiles,)), pltpu.SemaphoreType.DMA((n_cols,)), pltpu.SemaphoreType.DMA,
         pltpu.SemaphoreType.DMA((2,))],
    )(acts, w_qkv, w_o, cos_t, sin_t)


def attention_bwd(cot, w_qkv, w_o, q_rot, k_rot, v_raw, cos_t, sin_t, scale):
    n_rows, depth = cot.shape
    head = k_rot.shape[1]
    n_q, width = q_rot.shape[1], w_qkv.shape[1]
    n_rep = n_q // head
    tile = 256
    n_tiles = n_rows // tile

    def body(cot_hbm, w_hbm, wo_hbm, q, k, v, cos_ref, sin_ref, d_qkv, part_hbm,
             cot_v, w_v, wo_v, part_v, dk_acc, dv_acc, c_sem, w_sem, wo_sem, o_sem):
        order = list(reversed(range(n_tiles)))
        c_copy = [pltpu.make_async_copy(cot_hbm.at[pl.ds(i * tile, tile)], cot_v.at[pl.ds(i * tile, tile)],
                                        c_sem.at[i]) for i in range(n_tiles)]
        w_copy = pltpu.make_async_copy(w_hbm, w_v, w_sem)
        wo_copy = pltpu.make_async_copy(wo_hbm, wo_v, wo_sem)
        o_copy = [pltpu.make_async_copy(part_v.at[i % 2], part_hbm.at[pl.ds(i * tile, tile)], o_sem.at[i % 2])
                  for i in range(n_tiles)]
        for copy in [wo_copy] + [c_copy[i] for i in order[:1]] + [w_copy] + [c_copy[i] for i in order[1:]]:
            copy.start()
        wo_copy.wait()
        for n, i in enumerate(order):
            rows, end = pl.ds(i * tile, tile), (i + 1) * tile
            c_copy[i].wait()
            d_o = dot(cot_v[rows, :], wo_v[...], NT).astype(BF)
            q_rows = join([q[rows, pl.ds(h * head, head)] for h in range(n_rep)], 0)
            do_rows = join([d_o[:, h * head:(h + 1) * head] for h in range(n_rep)], 0)
            probs = causal_probs(q_rows, k, i * tile, tile, n_rep)
            d_probs = dot(do_rows, v[:end], NT)
            d_scores = (probs * (d_probs - jnp.sum(d_probs * probs, axis=1, keepdims=True))).astype(BF)
            dv_part = dot(probs.astype(BF), do_rows, TN)
            dk_part = dot(d_scores, q_rows, TN)
            if n == 0:
                dv_acc[...] = dv_part
                dk_acc[...] = dk_part
            else:
                dv_acc[:end] += dv_part
                dk_acc[:end] += dk_part
            dq_rows = dot(d_scores, k[:end], NN).astype(BF).astype(F32) * scale
            cos, sin = cos_ref[rows, :], sin_ref[rows, :]
            parts = [unrotate(dq_rows[h * tile:(h + 1) * tile], cos, sin).astype(BF) for h in range(n_rep)]
            parts.append(unrotate(dk_acc[rows, :].astype(BF).astype(F32), cos, sin).astype(BF))
            parts.append(dv_acc[rows, :].astype(BF))
            tile_grad = join(parts, 1)
            d_qkv[rows, :] = tile_grad
            if n == 0:
                w_copy.wait()
            if n >= 2:
                o_copy[i].wait()
            part_v[i % 2] = dot(tile_grad, w_v[...], NT).astype(BF)
            o_copy[i].start()
        for i in order[-2:]:
            o_copy[i].wait()

    any_spec = pl.BlockSpec(memory_space=pl.ANY)
    rest = (q_rot, k_rot, v_raw, cos_t, sin_t)
    outs = [jax.ShapeDtypeStruct((n_rows, width), BF), jax.ShapeDtypeStruct((n_rows, depth), BF)]
    return call(
        body, (1,), [any_spec] * 3 + [whole(r) for r in rest], [whole(outs[0]), any_spec], outs,
        2 * n_rows * depth * (width + n_q) + 8e9, 2 * (2 * n_rows * depth + depth * (width + n_q)),
        [pltpu.VMEM((n_rows, depth), BF), pltpu.VMEM(w_qkv.shape, BF), pltpu.VMEM(w_o.shape, BF),
         pltpu.VMEM((2, tile, depth), BF), pltpu.VMEM((n_rows, head), F32), pltpu.VMEM((n_rows, head), F32),
         pltpu.SemaphoreType.DMA((n_tiles,)), pltpu.SemaphoreType.DMA, pltpu.SemaphoreType.DMA,
         pltpu.SemaphoreType.DMA((2,))],
    )(cot, w_qkv, w_o, *rest)


def aligned(offset):
    return pl.multiple_of(offset, 128)


def act_cotangent(pieces, offsets, seq, w_down, gate, up, tile):
    width, depth = w_down.shape
    n_rows = sum(p.shape[1] for p in pieces)
    n_pieces = len(pieces)

    def body(off_ref, *refs):
        p_refs, (w_ref, g_ref, u_ref, dg_ref, du_ref) = refs[:n_pieces], refs[n_pieces:]
        rhs = w_ref[...]
        for group in ([0], [1], [2], [3, 4]):
            vals = dot(join([p_refs[g][...] for g in group], 0), rhs, NT).astype(BF)
            at = 0
            for g in group:
                size = p_refs[g].shape[0]
                rows = pl.ds(aligned(off_ref[g]), size)
                d_z = vals[at:at + size].astype(F32)
                at += size
                gate_v, up_v = g_ref[rows, :].astype(F32), u_ref[rows, :].astype(F32)
                square = gate_v * gate_v
                tanh = jnp.tanh(gate_v * (GELU_C + (GELU_C * GELU_A) * square))
                half = 0.5 + 0.5 * tanh
                slope = half + (0.5 * gate_v) * (1.0 - tanh * tanh) * (GELU_C + (3.0 * GELU_C * GELU_A) * square)
                du_ref[rows, :] = (d_z * (gate_v * half)).astype(BF)
                dg_ref[rows, :] = (d_z * up_v * slope).astype(BF)

    p_specs = [pl.BlockSpec((None,) + p.shape[1:], lambda i: (seq, 0, 0), pipeline_mode=pl.Buffered(1)) for p in pieces]
    o_spec = pl.BlockSpec((n_rows, tile), lambda i: (0, i))
    return call(
        body, (pl.cdiv(width, tile),),
        [pl.BlockSpec(memory_space=pltpu.SMEM)] + p_specs + [pl.BlockSpec((tile, depth), lambda i: (i, 0)), o_spec, o_spec],
        [o_spec] * 2, [jax.ShapeDtypeStruct((n_rows, width), BF)] * 2,
        2 * n_rows * depth * width, 2 * (n_rows * depth + depth * width + 4 * n_rows * width),
    )(offsets, *pieces, w_down, gate, up)


def down_grad(acts, pieces, offsets, tile):
    n_seq = len(acts)
    n_tok, width = acts[0].shape
    depth = pieces[0].shape[2]

    def body(off_ref, *refs):
        z_refs, p_refs, out = refs[:n_seq], refs[n_seq:-1], refs[-1]
        left = join([z[pl.ds(aligned(off_ref[g]), p.shape[1]), :] for z in z_refs for g, p in enumerate(p_refs)], 0)
        right = join([p[s] for s in range(n_seq) for p in p_refs], 0)
        out[...] = dot(left, right, TN).astype(BF)

    p_specs = [pl.BlockSpec(p.shape[:2] + (tile,), lambda i: (0, 0, i)) for p in pieces]
    return call(
        body, (depth // tile,),
        [pl.BlockSpec(memory_space=pltpu.SMEM)] + [whole(z) for z in acts] + p_specs,
        pl.BlockSpec((width, tile), lambda i: (0, i)), jax.ShapeDtypeStruct((width, depth), BF),
        2 * n_seq * n_tok * width * depth, 2 * (n_seq * n_tok * (width + depth) + width * depth),
    )(offsets, *acts, *pieces)


def gated_mlp(acts, w_gate, w_up):
    n_rows, depth = acts.shape
    width = w_gate.shape[1]
    tile, m_tile = 384, 256

    def body(a_ref, wg, wu, g_ref, u_ref, z_ref):
        rhs = jnp.concatenate([wg[...], wu[...]], axis=1)
        for start in range(0, n_rows, m_tile):
            rows = pl.ds(start, m_tile)
            both = dot(a_ref[rows, :], rhs, NN).astype(BF)
            g_ref[rows, :] = both[:, :tile]
            u_ref[rows, :] = both[:, tile:]
            gate = both[:, :tile].astype(F32)
            half = 0.5 + 0.5 * jnp.tanh(gate * (GELU_C + (GELU_C * GELU_A) * (gate * gate)))
            z_ref[rows, :] = (gate * half * both[:, tile:].astype(F32)).astype(BF)

    w_spec = pl.BlockSpec((depth, tile), lambda i: (0, i))
    o_spec = pl.BlockSpec((n_rows, tile), lambda i: (0, i))
    return call(
        body, (width // tile,), [whole(acts), w_spec, w_spec], [o_spec] * 3,
        [jax.ShapeDtypeStruct((n_rows, width), BF)] * 3,
        4 * n_rows * depth * width, 2 * (n_rows * depth + 2 * depth * width + 3 * n_rows * width),
    )(acts, w_gate, w_up)


def weight_grad(lhs, rhs_groups, out_widths, tile, stream):
    n_seq, n_tok = len(lhs), lhs[0].shape[0]
    n_out = lhs[0].shape[1]
    rhs = [r for group in rhs_groups for r in group]
    n_groups = len(rhs_groups)

    def body(*refs):
        l_refs, r_refs, o_refs = refs[:n_seq], refs[n_seq:n_seq + n_seq * n_groups], refs[n_seq + n_seq * n_groups:]
        left = join([l[...] for l in l_refs], 0)
        right = join([join([r_refs[g * n_seq + s][...] for s in range(n_seq)], 0) for g in range(n_groups)], 1)
        acc = dot(left, right, TN)
        at = 0
        for o in o_refs:
            o[...] = acc[:, at:at + o.shape[1]].astype(BF)
            at += o.shape[1]

    if stream == "rows":
        grid = (n_out // tile,)
        l_specs = [pl.BlockSpec((n_tok, tile), lambda i: (0, i)) for _ in lhs]
        r_specs = [whole(r) for r in rhs]
        o_specs = [pl.BlockSpec((tile, w), lambda i: (i, 0)) for w in out_widths]
    else:
        grid = (out_widths[0] // tile,)
        l_specs = [whole(l) for l in lhs]
        r_specs = [pl.BlockSpec((n_tok, tile), lambda i: (0, i)) for _ in rhs]
        o_specs = [pl.BlockSpec((n_out, tile), lambda i: (0, i)) for _ in out_widths]
    total = sum(out_widths)
    return call(
        body, grid, l_specs + r_specs, o_specs,
        [jax.ShapeDtypeStruct((n_out, w), BF) for w in out_widths],
        2 * n_seq * n_tok * n_out * total, 2 * (n_seq * n_tok * (n_out + total) + n_out * total),
    )(*lhs, *rhs)


def tp_sum(part, n_tp):
    def body(x_ref, out_ref, slots, send_sem, recv_sem):
        me = lax.axis_index("tp")
        barrier = pltpu.get_barrier_semaphore()
        for step in range(1, n_tp):
            pl.semaphore_signal(barrier, inc=1, device_id={"tp": lax.rem(me + step, n_tp)},
                                device_id_type=pl.DeviceIdType.MESH)
        pl.semaphore_wait(barrier, n_tp - 1)
        copies = []
        for step in range(1, n_tp):
            copies.append(pltpu.make_async_remote_copy(
                src_ref=x_ref, dst_ref=slots.at[me], send_sem=send_sem.at[step], recv_sem=recv_sem.at[step],
                device_id={"tp": lax.rem(me + step, n_tp)}, device_id_type=pl.DeviceIdType.MESH))
            copies[-1].start()
        slots[me] = x_ref[...]
        for copy in copies:
            copy.wait()
        total = slots[0]
        for step in range(1, n_tp):
            total = total + slots[step]
        out_ref[...] = total

    return pl.pallas_call(
        body,
        out_shape=jax.ShapeDtypeStruct(part.shape, F32),
        in_specs=[pl.BlockSpec(memory_space=pltpu.VMEM)],
        out_specs=pl.BlockSpec(memory_space=pltpu.VMEM),
        scratch_shapes=[pltpu.VMEM((n_tp,) + part.shape, F32), pltpu.SemaphoreType.DMA((n_tp,)),
                        pltpu.SemaphoreType.DMA((n_tp,))],
        compiler_params=pltpu.CompilerParams(collective_id=0, has_side_effects=True),
        cost_estimate=pl.CostEstimate(flops=5_000_000_000, bytes_accessed=1_000_000, transcendentals=0),
        name="tp_sum",
    )(part)


def solution(mesh):
    n_tp = mesh.shape["tp"]
    act_spec = P("dp", "tp", None)
    head_spec = P(None, "tp", None)
    in_specs = (act_spec, P("dp", None), head_spec, head_spec, head_spec, P("tp", None, None),
                P(None, "tp"), P(None, "tp"), P("tp", None), P(None), P(None), act_spec)
    out_specs = (act_spec, act_spec, P("dp", "tp", None), P("dp", "tp", None), P("dp", "tp", None),
                 P(("dp", "tp"), None, None), P("dp", "tp"), P("dp", "tp"), P(("dp", "tp"), None), P("dp"), P("dp"))

    def gather(part):
        return lax.all_gather(part, "tp", axis=0, tiled=True)

    def scatter(part):
        return lax.psum_scatter(part, "tp", scatter_dimension=0, tiled=True)

    def local_step(x_in, positions, w_q, w_k, w_v, w_o, w_gate, w_up, w_down, gain_attn, gain_mlp, d_out):
        n_seq = x_in.shape[0]
        seqs = range(n_seq)
        depth, n_rep, head = w_q.shape
        scale = head ** -0.5
        w_qkv = jnp.concatenate([w.reshape(depth, -1) for w in (w_q, w_k, w_v)], axis=1)
        wo2 = w_o.reshape(-1, depth)
        cos_t, sin_t = rope_tables(positions, head)

        x = [x_in[s] for s in seqs]
        d_y = [d_out[s] for s in seqs]
        latest = []

        def run(fn, first, *rest):
            out = fn(after(first, *latest), *rest)
            latest[:] = jax.tree.leaves(out)[:1]
            return out

        def norm(vals, gain):
            return jax.vjp(rms_norm, vals, gain)

        def mid_norm(proj, vals):
            total = (vals.astype(F32) + proj.astype(F32)).astype(BF)
            return norm(total, gain_mlp) + (total,)

        def mlp_grad(d_g, d_u):
            return rows_times_weights([d_g, d_u], [w_gate, w_up], "nt", 768)

        def norm_back(cot, pull, skip):
            d_vals, d_gain = pull(cot)
            return skip + d_vals, d_gain

        def add_out(part, vals):
            return (vals.astype(F32) + part.astype(F32)).astype(BF)

        none = [None] * n_seq
        normed_all, attn, attn_part, attn_proj, mlp_all = (list(none) for _ in range(5))
        norm_attn_pull, norm_mlp_pull, mlp_in, hidden, _, gated, d_mlp_in = (list(none) for _ in range(7))
        down_out, d_hidden, gain_mlp_part, d_hidden_all, d_qkv, d_normed = (list(none) for _ in range(6))
        grad_x, gain_attn_part = (list(none) for _ in range(2))

        n_chip = n_tp // 2
        me = lax.axis_index("tp")
        chip, core = me // 2, me % 2
        sibling = [(t, t ^ 1) for t in range(n_tp)]
        onward = [(t, 2 * ((t // 2 + 1 - 2 * (t % 2)) % n_chip) + t % 2) for t in range(n_tp)]
        share = d_out.shape[1]
        back = 2 * core - 1
        offsets = jnp.stack([2 * share * chip, 2 * share * ((chip + back) % n_chip), 2 * share * ((chip - back) % n_chip),
                             2 * share * ((chip + 2) % n_chip) + share * core,
                             2 * share * ((chip + 2) % n_chip) + share * (1 - core)]).astype(jnp.int32)

        def pair_up(mine, other):
            return jnp.where(core == 0, jnp.concatenate([mine, other], axis=1), jnp.concatenate([other, mine], axis=1))

        def own_half(vals):
            return lax.dynamic_slice_in_dim(vals, core * share, share, axis=1)

        dout_sib = lax.ppermute(d_out, "tp", sibling)
        for s in seqs:
            out, norm_attn_pull[s] = run(norm, x[s], gain_attn)
            normed_all[s] = gather(out)
        dout_pair = run(pair_up, d_out, dout_sib)
        for s in seqs:
            attn[s] = run(attention_fwd, normed_all[s], w_qkv, wo2, cos_t[s], sin_t[s], n_rep, head, scale)
            attn_part[s] = attn[s][4]
        attn_proj[0] = scatter(attn_part[0])
        dout_near = lax.ppermute(after(dout_pair, attn_part[1]), "tp", onward)

        def mid(s):
            mlp_in[s], norm_mlp_pull[s], hidden[s] = run(mid_norm, attn_proj[s], x[s])
            mlp_all[s] = gather(mlp_in[s])

        def mlp_main(s):
            gated[s] = run(gated_mlp, mlp_all[s], w_gate, w_up)

        def mlp_down(s):
            part = run(lambda z: rows_times_weights([z], [w_down], "nn", 768), gated[s][2])
            down_out[s] = scatter(part)

        d_gate, d_up, y_out = (list(none) for _ in range(3))
        mid(0)
        for s in seqs[1:]:
            attn_proj[s] = scatter(after(attn_part[s], mlp_in[0]))
        mlp_main(0)
        dout_pass = run(own_half, dout_near)
        dout_far = lax.ppermute(dout_pass, "tp", onward)
        dout_near2 = lax.ppermute(after(dout_near, dout_pass), "tp", sibling)
        mlp_down(0)
        dout_far2 = lax.ppermute(dout_far, "tp", sibling)
        dout_pieces = (dout_pair, dout_near, dout_near2, dout_far, dout_far2)
        mid(1)

        def act_grad(s):
            d_gate[s], d_up[s] = run(lambda off: act_cotangent(dout_pieces, off, s, w_down, *gated[s][:2], 512), offsets)

        def mlp_back(s):
            d_mlp_in[s] = scatter(run(mlp_grad, d_gate[s], d_up[s]))

        def mid_back(s):
            d_hidden[s], gain_mlp_part[s] = run(norm_back, d_mlp_in[s], norm_mlp_pull[s], d_y[s])
            d_hidden_all[s] = gather(d_hidden[s])

        def attn_back(s):
            d_qkv[s], part = run(attention_bwd, d_hidden_all[s], w_qkv, wo2, *attn[s][:3], cos_t[s], sin_t[s], scale)
            d_normed[s] = scatter(part)

        def last_back(s):
            grad_x[s], gain_attn_part[s] = run(norm_back, d_normed[s], norm_attn_pull[s], d_hidden[s])

        def add_out(part, vals):
            return (vals.astype(F32) + part.astype(F32)).astype(BF)

        act_grad(0)
        mlp_back(0)
        mlp_main(1)
        act_grad(1)
        y_out[0] = run(add_out, down_out[0], hidden[0])
        mid_back(0)
        mlp_back(1)
        mlp_down(1)
        attn_back(0)
        mid_back(1)
        act_out = [g[2] for g in gated]
        grad_wgate, grad_wup = run(lambda first: weight_grad(
            [first, mlp_all[1]], [d_gate, d_up], (w_gate.shape[1],) * 2, 384, "rows"), mlp_all[0])
        grad_wdown = run(lambda first: down_grad([first, act_out[1]], dout_pieces, offsets, 768), act_out[0])
        attn_back(1)
        (grad_wo,) = run(lambda first: weight_grad([first, attn[1][3]], [d_hidden_all], (depth,), 768, "cols"),
                         attn[0][3])
        grad_wq, grad_wk, grad_wv = run(lambda first: weight_grad(
            [first, normed_all[1]], [d_qkv], tuple(w[0].size for w in (w_q, w_k, w_v)), 384, "rows"),
            normed_all[0])
        y_out[1] = run(add_out, down_out[1], hidden[1])
        last_back(0)
        last_back(1)
        back_attn, back_mlp = gain_attn_part, gain_mlp_part
        gain_parts = jnp.stack([functools.reduce(jnp.add, back) for back in (back_attn, back_mlp)])
        gains = tp_sum(gain_parts, n_tp)
        return (jnp.stack(y_out), jnp.stack(grad_x), grad_wq.reshape(w_q.shape), grad_wk.reshape(w_k.shape),
                grad_wv.reshape(w_v.shape), grad_wo.reshape(w_o.shape), grad_wgate, grad_wup, grad_wdown,
                gains[0], gains[1])

    return jax.shard_map(local_step, mesh=mesh, in_specs=in_specs, out_specs=out_specs, check_vma=False)
```
